32 devices in a mesh: gx: 2 (over y), gy: 4 (over x, core), gz: 4 (over z).
Axes of the slice: x: 2, y: 2, z: 4, core: 2. Of those that a mesh axis runs over, the one named last changes fastest.
Arguments:
- right_side: float32 [16, 256, 512], P('gx', 'gy', 'gz'), may hold values from -4 to 4
- start: float32 [16, 256, 512], P('gx', 'gy', 'gz'), may hold values from -6 to 6
Outputs:
- solution: float32 [16, 256, 512], P('gx', 'gy', 'gz')
The draws below stay inside these ranges and needn't reach their ends.
All inputs are finite; a program needn't handle non-finite values.
Results may differ from the reference program's by a relative error of at most 0.0003.
Values sent between devices are 32-bit elements; how exact they have to be, the bound alone decides.
A program may use at most 128 MiB of HBM per device.

```python
import jax
import jax.numpy as jnp
from jax import lax

LEVELS = 4
SWEEPS = 2
CSWEEPS = 8
NX = 16
NY = 256
NZ = 512


def draw_right_side(key, part):
    values = jnp.clip(jax.random.normal(key, (NX, NY, NZ), jnp.float32), -4.0, 4.0)
    return values


def steps_of(key, shape, pieces, low, top_value):
    def one(axis_at, shards_of):
        draws = jax.random.uniform(jax.random.fold_in(jax.random.fold_in(key, 6), axis_at), (shards_of,), jnp.float32, low / len(pieces), top_value / len(pieces))
        return jnp.repeat(jnp.exp(draws), shape[axis_at] // shards_of).reshape((-1,) + (1,) * (len(shape) - axis_at - 1))

    factor_of = one(*pieces[0])
    for cut in pieces[1:]:
        factor_of = factor_of * one(*cut)
    return factor_of


def scatter_about(own_key, shape, deviation, reach, pieces=(), held_as=jnp.bfloat16):
    factor_of = steps_of(own_key, shape, pieces, -0.22, 0.18) if pieces else 1.0
    entries = jax.random.normal(own_key, shape, jnp.float32) * deviation * factor_of
    return jnp.minimum(jnp.maximum(entries, -reach), reach).astype(held_as)


def setup_inputs(seed: int = 0) -> dict:
    streams_of = jax.random.split(jax.random.key(seed), 3)
    right_side = draw_right_side(jax.random.fold_in(streams_of[2], 71), 0)
    start = scatter_about(streams_of[1], (NX, NY, NZ), 1.0, 6.0, ((0, 2), (1, 4), (2, 4)), jnp.float32)
    return {"right_side": right_side, "start": start}


def neighbours(padded):
    total = padded[2:, 1:-1, 1:-1] + padded[:-2, 1:-1, 1:-1]
    total = total + padded[1:-1, 2:, 1:-1] + padded[1:-1, :-2, 1:-1]
    return total + padded[1:-1, 1:-1, 2:] + padded[1:-1, 1:-1, :-2]


def parity(dims):
    first = lax.broadcasted_iota(jnp.int32, dims, 0)
    second = lax.broadcasted_iota(jnp.int32, dims, 1)
    third = lax.broadcasted_iota(jnp.int32, dims, 2)
    return (first + second + third) % 2


def smooth(correction, source, factor, colours, count):
    for pass_index in range(count):
        for colour in (0, 1):
            beside_all = neighbours(jnp.pad(correction, 1))
            correction = jnp.where(colours == colour, (factor * source + beside_all) / 6.0, correction)
    return correction


def restrict(residual):
    sx, sy, sz = residual.shape
    return residual.reshape(sx // 2, 2, sy // 2, 2, sz // 2, 2).mean(axis=(1, 3, 5))


def prolong(coarse):
    return jnp.repeat(jnp.repeat(jnp.repeat(coarse, 2, axis=0), 2, axis=1), 2, axis=2)


def reference(right_side, start):
    stored = []
    correction = start
    source = right_side
    for depth in range(LEVELS - 1):
        factor = 4.0 ** depth
        if depth > 0:
            correction = jnp.zeros_like(source)
        colours = parity(source.shape)
        correction = smooth(correction, source, factor, colours, SWEEPS)
        residual = source - (6.0 * correction - neighbours(jnp.pad(correction, 1))) / factor
        stored.append((correction, source, colours))
        source = restrict(residual)
    correction = smooth(jnp.zeros_like(source), source, 4.0 ** (LEVELS - 1), parity(source.shape), CSWEEPS)
    for depth in reversed(range(LEVELS - 1)):
        fine_value, fine_source, colours = stored[depth]
        correction = smooth(fine_value + prolong(correction), fine_source, 4.0 ** depth, colours, SWEEPS)
    return correction
```

```python
import functools

import jax
import jax.numpy as jnp
from jax import lax
from jax.experimental import pallas as pl
from jax.experimental.pallas import tpu as pltpu
from jax.sharding import PartitionSpec as P

MESH = pl.DeviceIdType.MESH
SIXTH = 1.0 / 6.0
PAD = 8
DOWN0 = 5
SIDE0 = 4
SIDE1 = 6
RHS1 = 5
CSWEEPS = 8


def dot(a, b):
    return jnp.dot(a, b, precision=lax.Precision.HIGHEST, preferred_element_type=jnp.float32)


def iota(shape, axis):
    return lax.broadcasted_iota(jnp.int32, shape, axis)


def beside(v, edge):
    rows, lanes = v.shape
    up = pltpu.roll(v, 1, axis=0) + pltpu.roll(v, rows - 1, axis=0)
    low = pltpu.roll(v, 1, axis=1)
    high = pltpu.roll(v, lanes - 1, axis=1)
    if edge:
        lane = iota(v.shape, 1)
        low = jnp.where(lane == 0, 0.0, low)
        high = jnp.where(lane == lanes - 1, 0.0, high)
    return up + (low + high)


def update(v_ref, b_ref, code, first, last, origin, colour, factor, edge=False):
    def body(i, carry):
        v = v_ref[i]
        total = (v_ref[i - 1] + v_ref[i + 1]) + beside(v, edge)
        want = lax.rem(i + origin + colour, 2)
        v_ref[i] = jnp.where(code[...] == want, (factor * b_ref[i] + total) * SIXTH, v)
        return carry

    lax.fori_loop(first, last, body, 0)


def residual(v_ref, b_ref, i, factor, edge=False):
    v = v_ref[i]
    total = (v_ref[i - 1] + v_ref[i + 1]) + beside(v, edge)
    return b_ref[i] - (6.0 * v - total) * (1.0 / factor)


class Exchange:
    def __init__(self, ref, sems, send, recv, box, depth, me, sizes):
        self.ref, self.sems, self.send, self.recv = ref, sems, send, recv
        self.c0, self.n, self.rows, self.l0, self.lanes = box
        self.depth, self.me, self.sizes = depth, me, sizes

    def _x(self):
        c0, n, depth = self.c0, self.n, self.depth
        gx = self.sizes[0]
        mx, my, mz = self.me
        rows = pl.ds(PAD, self.rows)
        width = 128
        out = []
        hop = 1
        slot = 0
        while (hop - 1) * n < depth and hop < gx:
            count = min(n, depth - (hop - 1) * n)
            far = (hop - 1) * n
            up = (c0 + n - count, c0 - far - count, mx + hop < gx, mx + hop, mx >= hop)
            down = (c0, c0 + n + far, mx >= hop, mx - hop, mx + hop < gx)
            for src, dst, may_send, peer, may_recv in (up, down):
                copy = pltpu.make_async_remote_copy(
                    src_ref=self.ref.at[pl.ds(src, count), rows, pl.ds(0, width)],
                    dst_ref=self.ref.at[pl.ds(dst, count), rows, pl.ds(0, width)],
                    send_sem=self.sems.at[0, slot],
                    recv_sem=self.sems.at[1, slot],
                    device_id=(peer, my, mz),
                    device_id_type=MESH,
                )
                out.append((copy, may_send, may_recv))
                slot += 1
            hop += 1
        return out

    def _y(self):
        gy = self.sizes[1]
        mx, my, mz = self.me
        planes = pl.ds(self.c0 - self.depth, self.n + 2 * self.depth)
        out = []
        up = (self.rows, 0, my + 1 < gy, my + 1, my >= 1)
        down = (PAD, PAD + self.rows, my >= 1, my - 1, my + 1 < gy)
        for k, (src, dst, may_send, peer, may_recv) in enumerate((up, down)):
            copy = pltpu.make_async_remote_copy(
                src_ref=self.ref.at[planes, pl.ds(src, PAD), pl.ds(0, 128)],
                dst_ref=self.ref.at[planes, pl.ds(dst, PAD), pl.ds(0, 128)],
                send_sem=self.sems.at[0, 4 + k],
                recv_sem=self.sems.at[1, 4 + k],
                device_id=(mx, peer, mz),
                device_id_type=MESH,
            )
            out.append((copy, may_send, may_recv))
        return out

    def _z(self):
        gz = self.sizes[2]
        mx, my, mz = self.me
        out = []
        up = (0, mz + 1 < gz, mz + 1, mz >= 1)
        down = (1, mz >= 1, mz - 1, mz + 1 < gz)
        for k, may_send, peer, may_recv in (up, down):
            copy = pltpu.make_async_remote_copy(
                src_ref=self.send.at[k],
                dst_ref=self.recv.at[k],
                send_sem=self.sems.at[0, 6 + k],
                recv_sem=self.sems.at[1, 6 + k],
                device_id=(mx, my, peer),
                device_id_type=MESH,
            )
            out.append((copy, may_send, may_recv))
        return out

    def _start(self, copies):
        for copy, may_send, may_recv in copies:
            pl.when(may_send)(copy.start)

    def _wait(self, copies):
        for copy, may_send, may_recv in copies:
            pl.when(may_send)(copy.wait_send)
            pl.when(may_recv)(copy.wait_recv)

    def start_x(self):
        self._start(self._x())

    def wait_x(self):
        self._wait(self._x())

    def start_y(self):
        self._start(self._y())

    def wait_y(self):
        self._wait(self._y())

    def _planes(self):
        return range(self.c0 - self.depth, self.c0 + self.n + self.depth)

    def start_z(self):
        d = self.depth
        shape = self.send.shape[1:]
        lane = iota(shape, 1)
        up = jnp.zeros(shape, jnp.float32)
        down = jnp.zeros(shape, jnp.float32)
        for k, i in enumerate(self._planes()):
            v = self.ref[i, :, 0:128]
            here = (lane >= k * d) & (lane < k * d + d)
            up = jnp.where(here, pltpu.roll(v, (k * d - (self.l0 + self.lanes - d)) % 128, axis=1), up)
            down = jnp.where(here, pltpu.roll(v, (k * d - self.l0) % 128, axis=1), down)
        self.send[0] = up
        self.send[1] = down
        self._start(self._z())

    def wait_z(self):
        self._wait(self._z())
        d = self.depth
        gz = self.sizes[2]
        mz = self.me[2]
        shape = self.recv.shape[1:]
        lane = iota(shape, 1)
        low_at = (self.l0 - d) % 128
        high_at = (self.l0 + self.lanes) % 128
        is_low = (lane >= low_at) & (lane < low_at + d)
        is_high = (lane >= high_at) & (lane < high_at + d)
        low_buffer = jnp.where(mz >= 1, self.recv[0], 0.0)
        high_buffer = jnp.where(mz + 1 < gz, self.recv[1], 0.0)
        whole = self.ref.shape[2] == 256
        for k, i in enumerate(self._planes()):
            low = pltpu.roll(low_buffer, (low_at - k * d) % 128, axis=1)
            high = pltpu.roll(high_buffer, (high_at - k * d) % 128, axis=1)
            if whole:
                self.ref[i, :, 128:256] = jnp.where(is_low, low, jnp.where(is_high, high, 0.0))
            else:
                v = self.ref[i]
                self.ref[i] = jnp.where(is_low, low, jnp.where(is_high, high, v))


def kernel(
    sizes, rhs_ref, start_ref, out_ref,
    e0, b0, f0, e1, b1, f1, v2, b2, v3, b3,
    t0, t1, t2, t3, w0, w1, w2, pack, slots,
    za, zb, zc, zd, ze, halo_sems, gather_sems,
):
    gx, gy, gz = sizes
    count = gx * gy * gz
    me = mx, my, mz = lax.axis_index("gx"), lax.axis_index("gy"), lax.axis_index("gz")
    mine = (mx * gy + my) * gz + mz
    lx, ly, lz = rhs_ref.shape
    c0, c1 = DOWN0 + 1, SIDE1 + 2
    hx, hy, hz = lx // 2, ly // 2, lz // 2
    qx, qy, qz = hx // 2, hy // 2, hz // 2
    x2, y2, z2 = gx * qx, gy * qy, gz * qz
    x3, y3, z3 = x2 // 2, y2 // 2, z2 // 2
    z3p = v3.shape[2]
    left = (128 - hz) // 2

    def coords(d):
        return (d // (gy * gz), lax.rem(d // gz, gy), lax.rem(d, gz))

    for ref in (e1, b1, f1, v2, v3):
        ref[...] = jnp.zeros_like(ref)
    rows0 = e0.shape[1]
    for ref in (e0, b0, f0):
        ref[:, 0:PAD, :] = jnp.zeros((ref.shape[0], PAD, 256), jnp.float32)
        ref[:, PAD + ly:, :] = jnp.zeros((ref.shape[0], PAD, 256), jnp.float32)
        for i in list(range(c0)) + list(range(c0 + lx, ref.shape[0])):
            ref[i] = jnp.zeros(ref.shape[1:], jnp.float32)

    barrier = pltpu.get_barrier_semaphore()

    def greet(k, carry):
        d = lax.rem(mine + k, count)
        pl.semaphore_signal(barrier, inc=1, device_id=coords(d), device_id_type=MESH)
        return carry

    lax.fori_loop(1, count, greet, 0)

    e0[c0:c0 + lx, PAD:PAD + ly, 0:128] = start_ref[...]
    b0[c0:c0 + lx, PAD:PAD + ly, 0:128] = rhs_ref[...]

    def code(shape, row0, lane_of, bounds):
        y = iota(shape, 0) + row0
        z = lane_of(iota(shape, 1))
        inside = (y >= 0) & (y < bounds[0]) & (z >= 0) & (z < bounds[1])
        return jnp.where(inside, (y + z) & 1, 5)

    t0[...] = code(t0.shape, my * ly - PAD, lambda c: mz * lz + jnp.where(c < 192, c, c - 256), (gy * ly, gz * lz))
    t1[...] = code(t1.shape, my * hy - PAD, lambda c: mz * hz + c - left, (gy * hy, gz * hz))
    t2[...] = code(t2.shape, -PAD, lambda c: c, (y2, z2))
    t3[...] = code(t3.shape, -PAD, lambda c: c, (y3, z3))

    pl.semaphore_wait(barrier, count - 1)

    box0 = (c0, lx, ly, 0, lz)
    box1 = (c1, hx, hy, left, hz)
    xe0 = Exchange(e0, halo_sems.at[0], za.at[0], za.at[1], box0, DOWN0, me, sizes)
    xb0 = Exchange(b0, halo_sems.at[1], zb.at[0], zb.at[1], box0, DOWN0 - 1, me, sizes)
    xf0 = Exchange(f0, halo_sems.at[2], zc.at[0], zc.at[1], box0, SIDE0, me, sizes)
    xb1 = Exchange(b1, halo_sems.at[3], zd.at[0], zd.at[1], box1, RHS1, me, sizes)
    xf1 = Exchange(f1, halo_sems.at[4], ze.at[0], ze.at[1], box1, SIDE1, me, sizes)

    xe0.start_x()
    xb0.start_x()
    xe0.wait_x()
    xe0.start_y()
    xb0.wait_x()
    xb0.start_y()
    xe0.wait_y()
    xe0.start_z()
    xb0.wait_y()
    xb0.start_z()
    xe0.wait_z()
    xb0.wait_z()

    def span(c, n, depth):
        return (
            jnp.maximum(c - depth, c - mx * n),
            jnp.minimum(c + n + depth, c + (gx - mx) * n),
        )

    for step in range(4):
        first, last = span(c0, lx, 4 - step)
        update(e0, b0, t0, first, last, mx * lx + c0, step % 2, 1.0)

    def pair0(j, carry):
        i = c0 + 2 * j
        r = residual(e0, b0, i, 1.0) + residual(e0, b0, i + 1, 1.0)
        w0[pl.ds(pl.multiple_of(j * ly, 8), ly), :] = r[PAD:PAD + ly, 0:128]
        return carry

    lax.fori_loop(0, hx, pair0, 0)
    r = w0[pl.ds(0, hx * hy, stride=2), :] + w0[pl.ds(1, hx * hy, stride=2), :]
    fold = jnp.where(iota((128, 128), 1) == left + iota((128, 128), 0) // 2, 0.125, 0.0)
    r = dot(r, fold)
    for j in range(hx):
        b1[c1 + j, PAD:PAD + hy, :] = r[j * hy:(j + 1) * hy]

    xb1.start_x()
    f0[c0:c0 + lx, PAD:PAD + ly, 0:128] = e0[c0:c0 + lx, PAD:PAD + ly, 0:128]
    xb1.wait_x()
    xb1.start_y()
    xf0.start_x()
    xb1.wait_y()
    xb1.start_z()
    xf0.wait_x()
    xf0.start_y()
    xb1.wait_z()

    for step in range(4):
        first, last = span(c1, hx, 4 - step)
        update(e1, b1, t1, first, last, mx * hx + c1, step % 2, 4.0)

    for j in range(qx):
        i = c1 + 2 * j
        r = residual(e1, b1, i, 4.0) + residual(e1, b1, i + 1, 4.0)
        w1[j * hy:(j + 1) * hy, :] = r[PAD:PAD + hy]
    r = w1[pl.ds(0, qx * qy, stride=2), :] + w1[pl.ds(1, qx * qy, stride=2), :]
    tiles = qx * qy // 8
    total = None
    for t in range(tiles):
        source = iota((128, 128), 0) - left
        target = iota((128, 128), 1)
        inside = (source >= 0) & (source < hz)
        fold = jnp.where(inside & (target == t * qz + source // 2), 0.125, 0.0)
        part = dot(r[8 * t:8 * t + 8], fold)
        total = part if total is None else total + part
    pack[...] = total
    slots[mine] = total

    def gather(k):
        d = lax.rem(mine + k, count)
        return pltpu.make_async_remote_copy(
            src_ref=pack,
            dst_ref=slots.at[mine],
            send_sem=gather_sems.at[0, d],
            recv_sem=gather_sems.at[1, mine],
            device_id=coords(d),
            device_id_type=MESH,
        )

    def gather_start(k, carry):
        gather(k).start()
        return carry

    lax.fori_loop(1, count, gather_start, 0)

    f1[c1:c1 + hx, PAD:PAD + hy, :] = e1[c1:c1 + hx, PAD:PAD + hy, :]
    xf1.start_x()
    xf0.wait_y()
    xf0.start_z()
    xf1.wait_x()
    xf1.start_y()

    def gather_wait(k, carry):
        d = lax.rem(mine + k, count)
        copy = pltpu.make_async_remote_copy(
            src_ref=pack,
            dst_ref=slots.at[d],
            send_sem=gather_sems.at[0, d],
            recv_sem=gather_sems.at[1, d],
            device_id=coords(d),
            device_id_type=MESH,
        )
        copy.wait_send()
        copy.wait_recv()
        return carry

    lax.fori_loop(1, count, gather_wait, 0)
    xf1.wait_y()
    xf1.start_z()

    per = 128 // qz
    b2[...] = jnp.zeros_like(b2)

    def spread(c, carry):
        cx, cy = c // gy, lax.rem(c, gy)
        lane = iota((8, 128), 1)
        for g in range(gz // per):
            parts = [slots[c * gz + g * per + q] for q in range(per)]
            for t in range(tiles):
                p, h = t // (qy // 8), t % (qy // 8)
                tile = jnp.zeros((8, 128), jnp.float32)
                for q in range(per):
                    here = (lane >= q * qz) & (lane < (q + 1) * qz)
                    tile = jnp.where(here, pltpu.roll(parts[q], ((q - t) * qz) % 128, axis=1), tile)
                rows = pl.ds(pl.multiple_of(PAD + cy * qy + 8 * h, 8), 8)
                b2[1 + cx * qx + p, rows, 128 * g:128 * (g + 1)] = tile
        return carry

    lax.fori_loop(0, gx * gy, spread, 0)

    for step in range(4):
        update(v2, b2, t2, 1, 1 + x2, 1, step % 2, 16.0, True)

    def pair2(q, carry):
        r = residual(v2, b2, 1 + 2 * q, 16.0, True) + residual(v2, b2, 2 + 2 * q, 16.0, True)
        for g in range(z2 // 128):
            w2[g] = r[:, 128 * g:128 * (g + 1)]
        half = y2 // 2
        r = jnp.concatenate(
            [
                w2[g, pl.ds(PAD, half, stride=2), :] + w2[g, pl.ds(PAD + 1, half, stride=2), :]
                for g in range(z2 // 128)
            ],
            axis=1,
        )
        fold = jnp.where(iota((z2, z3p), 1) == iota((z2, z3p), 0) // 2, 0.125, 0.0)
        b3[1 + q, PAD:PAD + half, :] = dot(r, fold)
        return carry

    b3[...] = jnp.zeros_like(b3)
    lax.fori_loop(0, x3, pair2, 0)

    def sweep3(k, carry):
        for colour in (0, 1):
            update(v3, b3, t3, 1, 1 + x3, 1, colour, 64.0, True)
        return carry

    lax.fori_loop(0, CSWEEPS, sweep3, 0)

    def lift3(q, carry):
        half = (y2 + 2 * PAD) // 2
        grow = jnp.where(iota((z3p, z2), 0) == iota((z3p, z2), 1) // 2, 1.0, 0.0)
        v = dot(v3[1 + q, PAD // 2:PAD // 2 + half, :], grow)
        for g in range(z2 // 128):
            w2[g, pl.ds(0, half, stride=2), :] = v[:, 128 * g:128 * (g + 1)]
            w2[g, pl.ds(1, half, stride=2), :] = v[:, 128 * g:128 * (g + 1)]
        for g in range(z2 // 128):
            lanes = slice(128 * g, 128 * (g + 1))
            for i in (1 + 2 * q, 2 + 2 * q):
                v2[i, :, lanes] = v2[i, :, lanes] + w2[g]
        return carry

    lax.fori_loop(0, x3, lift3, 0)

    for step in range(4):
        update(v2, b2, t2, 1, 1 + x2, 1, step % 2, 16.0, True)

    xf1.wait_z()
    rows1 = f1.shape[1]
    grow1 = jnp.where(
        iota((z2, 128), 0) == mz * qz + (iota((z2, 128), 1) - left + 2 * 128) // 2 - 128, 1.0, 0.0
    )
    rows2 = pl.ds(pl.multiple_of(my * qy, 8), rows1 // 2 + PAD)

    def lift2(i, carry):
        q = (mx * hx + i - c1) // 2
        v = dot(v2[1 + q, rows2, :][PAD // 2:PAD // 2 + rows1 // 2], grow1)
        w1[pl.ds(0, rows1 // 2, stride=2), :] = v
        w1[pl.ds(1, rows1 // 2, stride=2), :] = v
        f1[i] = f1[i] + w1[0:rows1, :]
        return carry

    first, last = span(c1, hx, SIDE1)
    lax.fori_loop(first, last, lift2, 0)

    for step in range(4):
        first, last = span(c1, hx, 5 - step)
        update(f1, b1, t1, first, last, mx * hx + c1, step % 2, 4.0)

    xf0.wait_z()
    grow0 = jnp.where(
        iota((128, 256), 0) == (left + iota((128, 256), 1) // 2) % 128, 1.0, 0.0
    )
    half0 = rows0 // 2

    def lift1(j, carry):
        v = dot(f1[j, PAD // 2:PAD // 2 + half0, :], grow0)
        i = c0 + 2 * (j - c1)
        for g in range(2):
            lanes = slice(128 * g, 128 * (g + 1))
            w0[pl.ds(0, half0, stride=2), :] = v[:, lanes]
            w0[pl.ds(1, half0, stride=2), :] = v[:, lanes]
            for k in (i, i + 1):
                f0[k, :, lanes] = f0[k, :, lanes] + w0[0:rows0, :]
        return carry

    first, last = span(c1, hx, SIDE0 // 2)
    lax.fori_loop(first, last, lift1, 0)

    for step in range(4):
        first, last = span(c0, lx, 3 - step)
        update(f0, b0, t0, first, last, mx * lx + c0, step % 2, 1.0)

    out_ref[...] = f0[c0:c0 + lx, PAD:PAD + ly, 0:128]


def local(sizes, right_side, start):
    gx, gy, gz = sizes
    lx, ly, lz = right_side.shape
    c0, c1 = DOWN0 + 1, SIDE1 + 2
    n0, n1 = lx + 2 * c0, lx // 2 + 2 * c1
    r0, r1 = ly + 2 * PAD, ly // 2 + 2 * PAD
    x2, y2, z2 = gx * lx // 4, gy * ly // 4, gz * lz // 4
    x3, y3, z3 = x2 // 2, y2 // 2, z2 // 2
    z3p = -(-z3 // 128) * 128
    f32, i32 = jnp.float32, jnp.int32
    count = gx * gy * gz
    return pl.pallas_call(
        functools.partial(kernel, sizes),
        out_shape=jax.ShapeDtypeStruct(start.shape, f32),
        in_specs=[pl.BlockSpec(memory_space=pltpu.VMEM)] * 2,
        out_specs=pl.BlockSpec(memory_space=pltpu.VMEM),
        scratch_shapes=[
            pltpu.VMEM((n0, r0, 256), f32),
            pltpu.VMEM((n0, r0, 256), f32),
            pltpu.VMEM((n0, r0, 256), f32),
            pltpu.VMEM((n1, r1, 128), f32),
            pltpu.VMEM((n1, r1, 128), f32),
            pltpu.VMEM((n1, r1, 128), f32),
            pltpu.VMEM((x2 + 2, y2 + 2 * PAD, z2), f32),
            pltpu.VMEM((x2 + 2, y2 + 2 * PAD, z2), f32),
            pltpu.VMEM((x3 + 2, y3 + 2 * PAD, z3p), f32),
            pltpu.VMEM((x3 + 2, y3 + 2 * PAD, z3p), f32),
            pltpu.VMEM((r0, 256), i32),
            pltpu.VMEM((r1, 128), i32),
            pltpu.VMEM((y2 + 2 * PAD, z2), i32),
            pltpu.VMEM((y3 + 2 * PAD, z3p), i32),
            pltpu.VMEM((lx // 2 * ly, 128), f32),
            pltpu.VMEM((max(lx // 4 * ly // 2, r1), 128), f32),
            pltpu.VMEM((z2 // 128, y2 + 2 * PAD, 128), f32),
            pltpu.VMEM((8, 128), f32),
            pltpu.VMEM((count, 8, 128), f32),
            pltpu.VMEM((2, 2, r0, 128), f32),
            pltpu.VMEM((2, 2, r0, 128), f32),
            pltpu.VMEM((2, 2, r0, 128), f32),
            pltpu.VMEM((2, 2, r1, 128), f32),
            pltpu.VMEM((2, 2, r1, 128), f32),
            pltpu.SemaphoreType.DMA((5, 2, 8)),
            pltpu.SemaphoreType.DMA((2, count)),
        ],
        compiler_params=pltpu.CompilerParams(
            collective_id=0, has_side_effects=True, vmem_limit_bytes=60 * 1024 * 1024
        ),
    )(right_side, start)


def solution(mesh):
    sizes = (mesh.shape["gx"], mesh.shape["gy"], mesh.shape["gz"])
    spec = P("gx", "gy", "gz")
    return jax.shard_map(
        functools.partial(local, sizes), mesh=mesh, in_specs=(spec, spec), out_specs=spec, check_vma=False
    )
```

```python
import functools

import jax
import jax.numpy as jnp
from jax import lax
from jax.experimental import pallas as pl
from jax.experimental.pallas import tpu as pltpu
from jax.sharding import PartitionSpec as P

MESH = pl.DeviceIdType.MESH
SIXTH = 1.0 / 6.0
PAD = 8
DOWN0 = 5
SIDE0 = 4
SIDE1 = 6
RHS1 = 5
CSWEEPS = 8


def dot(a, b):
    return jnp.dot(a, b, precision=lax.Precision.HIGHEST, preferred_element_type=jnp.float32)


def iota(shape, axis):
    return lax.broadcasted_iota(jnp.int32, shape, axis)


def beside(v, edge):
    rows, lanes = v.shape
    up = pltpu.roll(v, 1, axis=0) + pltpu.roll(v, rows - 1, axis=0)
    low = pltpu.roll(v, 1, axis=1)
    high = pltpu.roll(v, lanes - 1, axis=1)
    if edge:
        lane = iota(v.shape, 1)
        low = jnp.where(lane == 0, 0.0, low)
        high = jnp.where(lane == lanes - 1, 0.0, high)
    return up + (low + high)


def update(v_ref, b_ref, code, first, last, origin, colour, factor, edge=False, chunk=4):
    def some(start, size):
        planes = [v_ref[start - 1 + k] for k in range(size + 2)]
        sides = [beside(planes[k + 1], edge) for k in range(size)]
        fresh = []
        for k in range(size):
            total = (planes[k] + planes[k + 2]) + sides[k]
            want = lax.rem(start + (k + origin + colour), 2)
            value = (factor * b_ref[start + k] + total) * SIXTH
            fresh.append(jnp.where(code[...] == want, value, planes[k + 1]))
        for k in range(size):
            v_ref[start + k] = fresh[k]

    if isinstance(first, int) and last - first <= chunk:
        some(first, last - first)
        return

    def body(c, carry):
        some(jnp.minimum(first + c * chunk, last - chunk), chunk)
        return carry

    lax.fori_loop(0, (last - first + chunk - 1) // chunk, body, 0)


def residual(v_ref, b_ref, i, factor, edge=False):
    v = v_ref[i]
    total = (v_ref[i - 1] + v_ref[i + 1]) + beside(v, edge)
    return b_ref[i] - (6.0 * v - total) * (1.0 / factor)


class Exchange:
    def __init__(self, ref, sems, send, recv, box, depth, me, sizes):
        self.ref, self.sems, self.send, self.recv = ref, sems, send, recv
        self.c0, self.n, self.rows, self.l0, self.lanes = box
        self.depth, self.me, self.sizes = depth, me, sizes

    def _x(self):
        c0, n, depth = self.c0, self.n, self.depth
        gx = self.sizes[0]
        mx, my, mz = self.me
        rows = pl.ds(PAD, self.rows)
        width = 128
        out = []
        hop = 1
        slot = 0
        while (hop - 1) * n < depth and hop < gx:
            count = min(n, depth - (hop - 1) * n)
            far = (hop - 1) * n
            up = (c0 + n - count, c0 - far - count, mx + hop < gx, mx + hop, mx >= hop)
            down = (c0, c0 + n + far, mx >= hop, mx - hop, mx + hop < gx)
            for src, dst, may_send, peer, may_recv in (up, down):
                copy = pltpu.make_async_remote_copy(
                    src_ref=self.ref.at[pl.ds(src, count), rows, pl.ds(0, width)],
                    dst_ref=self.ref.at[pl.ds(dst, count), rows, pl.ds(0, width)],
                    send_sem=self.sems.at[0, slot],
                    recv_sem=self.sems.at[1, slot],
                    device_id=(peer, my, mz),
                    device_id_type=MESH,
                )
                out.append((copy, may_send, may_recv))
                slot += 1
            hop += 1
        return out

    def _y(self):
        gy = self.sizes[1]
        mx, my, mz = self.me
        planes = pl.ds(self.c0 - self.depth, self.n + 2 * self.depth)
        out = []
        up = (self.rows, 0, my + 1 < gy, my + 1, my >= 1)
        down = (PAD, PAD + self.rows, my >= 1, my - 1, my + 1 < gy)
        for k, (src, dst, may_send, peer, may_recv) in enumerate((up, down)):
            copy = pltpu.make_async_remote_copy(
                src_ref=self.ref.at[planes, pl.ds(src, PAD), pl.ds(0, 128)],
                dst_ref=self.ref.at[planes, pl.ds(dst, PAD), pl.ds(0, 128)],
                send_sem=self.sems.at[0, 4 + k],
                recv_sem=self.sems.at[1, 4 + k],
                device_id=(mx, peer, mz),
                device_id_type=MESH,
            )
            out.append((copy, may_send, may_recv))
        return out

    def _z(self):
        gz = self.sizes[2]
        mx, my, mz = self.me
        out = []
        up = (0, mz + 1 < gz, mz + 1, mz >= 1)
        down = (1, mz >= 1, mz - 1, mz + 1 < gz)
        for k, may_send, peer, may_recv in (up, down):
            copy = pltpu.make_async_remote_copy(
                src_ref=self.send.at[k],
                dst_ref=self.recv.at[k],
                send_sem=self.sems.at[0, 6 + k],
                recv_sem=self.sems.at[1, 6 + k],
                device_id=(mx, my, peer),
                device_id_type=MESH,
            )
            out.append((copy, may_send, may_recv))
        return out

    def _start(self, copies):
        for copy, may_send, may_recv in copies:
            pl.when(may_send)(copy.start)

    def _wait(self, copies):
        for copy, may_send, may_recv in copies:
            pl.when(may_send)(copy.wait_send)
            pl.when(may_recv)(copy.wait_recv)

    def start_x(self):
        self._start(self._x())

    def wait_x(self):
        self._wait(self._x())

    def start_y(self):
        self._start(self._y())

    def wait_y(self):
        self._wait(self._y())

    def _planes(self):
        return range(self.c0 - self.depth, self.c0 + self.n + self.depth)

    def start_z(self):
        d = self.depth
        shape = self.send.shape[1:]
        lane = iota(shape, 1)
        up = jnp.zeros(shape, jnp.float32)
        down = jnp.zeros(shape, jnp.float32)
        for k, i in enumerate(self._planes()):
            v = self.ref[i, :, 0:128]
            here = (lane >= k * d) & (lane < k * d + d)
            up = jnp.where(here, pltpu.roll(v, (k * d - (self.l0 + self.lanes - d)) % 128, axis=1), up)
            down = jnp.where(here, pltpu.roll(v, (k * d - self.l0) % 128, axis=1), down)
        self.send[0] = up
        self.send[1] = down
        self._start(self._z())

    def wait_z(self):
        self._wait(self._z())
        d = self.depth
        gz = self.sizes[2]
        mz = self.me[2]
        shape = self.recv.shape[1:]
        lane = iota(shape, 1)
        low_at = (self.l0 - d) % 128
        high_at = (self.l0 + self.lanes) % 128
        is_low = (lane >= low_at) & (lane < low_at + d)
        is_high = (lane >= high_at) & (lane < high_at + d)
        low_buffer = jnp.where(mz >= 1, self.recv[0], 0.0)
        high_buffer = jnp.where(mz + 1 < gz, self.recv[1], 0.0)
        whole = self.ref.shape[2] == 256
        for k, i in enumerate(self._planes()):
            low = pltpu.roll(low_buffer, (low_at - k * d) % 128, axis=1)
            high = pltpu.roll(high_buffer, (high_at - k * d) % 128, axis=1)
            if whole:
                self.ref[i, :, 128:256] = jnp.where(is_low, low, jnp.where(is_high, high, 0.0))
            else:
                v = self.ref[i]
                self.ref[i] = jnp.where(is_low, low, jnp.where(is_high, high, v))


def kernel(
    sizes, rhs_ref, start_ref, out_ref,
    e0, b0, f0, e1, b1, f1, v2, b2, v3, b3,
    t0, t1, t2, t3, w0, w1, w2, pack, slots,
    za, zb, zc, zd, ze, halo_sems, gather_sems,
):
    gx, gy, gz = sizes
    count = gx * gy * gz
    me = mx, my, mz = lax.axis_index("gx"), lax.axis_index("gy"), lax.axis_index("gz")
    mine = (mx * gy + my) * gz + mz
    lx, ly, lz = rhs_ref.shape
    c0, c1 = DOWN0 + 1, SIDE1 + 2
    hx, hy, hz = lx // 2, ly // 2, lz // 2
    qx, qy, qz = hx // 2, hy // 2, hz // 2
    x2, y2, z2 = gx * qx, gy * qy, gz * qz
    x3, y3, z3 = x2 // 2, y2 // 2, z2 // 2
    z3p = v3.shape[2]
    left = (128 - hz) // 2

    def coords(k):
        steps = (k // (gy * gz), k // gz % gy, k % gz)
        moved = [at + step for at, step in zip(me, steps)]
        return tuple(jnp.where(at >= size, at - size, at) for at, size in zip(moved, sizes))

    def number(at):
        return (at[0] * gy + at[1]) * gz + at[2]

    def others(body):
        if count <= 64:
            for k in range(1, count):
                body(k, 0)
        else:
            lax.fori_loop(1, count, body, 0)

    for ref in (e1, b1, f1, v2, v3):
        ref[...] = jnp.zeros_like(ref)
    rows0 = e0.shape[1]
    for ref in (e0, b0, f0):
        ref[:, 0:PAD, :] = jnp.zeros((ref.shape[0], PAD, 256), jnp.float32)
        ref[:, PAD + ly:, :] = jnp.zeros((ref.shape[0], PAD, 256), jnp.float32)
        for i in list(range(c0)) + list(range(c0 + lx, ref.shape[0])):
            ref[i] = jnp.zeros(ref.shape[1:], jnp.float32)

    barrier = pltpu.get_barrier_semaphore()

    def greet(k, carry):
        pl.semaphore_signal(barrier, inc=1, device_id=coords(k), device_id_type=MESH)
        return carry

    others(greet)

    e0[c0:c0 + lx, PAD:PAD + ly, 0:128] = start_ref[...]
    b0[c0:c0 + lx, PAD:PAD + ly, 0:128] = rhs_ref[...]

    def code(shape, row0, lane_of, bounds):
        y = iota(shape, 0) + row0
        z = lane_of(iota(shape, 1))
        inside = (y >= 0) & (y < bounds[0]) & (z >= 0) & (z < bounds[1])
        return jnp.where(inside, (y + z) & 1, 5)

    t0[...] = code(t0.shape, my * ly - PAD, lambda c: mz * lz + jnp.where(c < 192, c, c - 256), (gy * ly, gz * lz))
    t1[...] = code(t1.shape, my * hy - PAD, lambda c: mz * hz + c - left, (gy * hy, gz * hz))
    t2[...] = code(t2.shape, -PAD, lambda c: c, (y2, z2))
    t3[...] = code(t3.shape, -PAD, lambda c: c, (y3, z3))

    pl.semaphore_wait(barrier, count - 1)

    box0 = (c0, lx, ly, 0, lz)
    box1 = (c1, hx, hy, left, hz)
    xe0 = Exchange(e0, halo_sems.at[0], za.at[0], za.at[1], box0, DOWN0, me, sizes)
    xb0 = Exchange(b0, halo_sems.at[1], zb.at[0], zb.at[1], box0, DOWN0 - 1, me, sizes)
    xf0 = Exchange(f0, halo_sems.at[2], zc.at[0], zc.at[1], box0, SIDE0, me, sizes)
    xb1 = Exchange(b1, halo_sems.at[3], zd.at[0], zd.at[1], box1, RHS1, me, sizes)
    xf1 = Exchange(f1, halo_sems.at[4], ze.at[0], ze.at[1], box1, SIDE1, me, sizes)

    xe0.start_x()
    xb0.start_x()
    xe0.wait_x()
    xe0.start_y()
    xb0.wait_x()
    xb0.start_y()
    xe0.wait_y()
    xe0.start_z()
    xb0.wait_y()
    xb0.start_z()
    xe0.wait_z()
    xb0.wait_z()

    def span(c, n, depth):
        return (
            jnp.maximum(c - depth, c - mx * n),
            jnp.minimum(c + n + depth, c + (gx - mx) * n),
        )

    for step in range(4):
        first, last = span(c0, lx, 4 - step)
        update(e0, b0, t0, first, last, mx * lx + c0, step % 2, 1.0)

    def pair0(j, carry):
        i = c0 + 2 * j
        r = residual(e0, b0, i, 1.0) + residual(e0, b0, i + 1, 1.0)
        w0[j * ly:(j + 1) * ly, :] = r[PAD:PAD + ly, 0:128]
        return carry

    for j in range(hx):
        pair0(j, 0)
    r = w0[pl.ds(0, hx * hy, stride=2), :] + w0[pl.ds(1, hx * hy, stride=2), :]
    fold = jnp.where(iota((128, 128), 1) == left + iota((128, 128), 0) // 2, 0.125, 0.0)
    r = dot(r, fold)
    for j in range(hx):
        b1[c1 + j, PAD:PAD + hy, :] = r[j * hy:(j + 1) * hy]

    xb1.start_x()
    f0[c0:c0 + lx, PAD:PAD + ly, 0:128] = e0[c0:c0 + lx, PAD:PAD + ly, 0:128]
    xb1.wait_x()
    xb1.start_y()
    xf0.start_x()
    xb1.wait_y()
    xb1.start_z()
    xb1.wait_z()

    for step in range(4):
        first, last = span(c1, hx, 4 - step)
        update(e1, b1, t1, first, last, mx * hx + c1, step % 2, 4.0)

    for j in range(qx):
        i = c1 + 2 * j
        r = residual(e1, b1, i, 4.0) + residual(e1, b1, i + 1, 4.0)
        w1[j, 0:hy, :] = r[PAD:PAD + hy]
    r = jnp.concatenate(
        [w1[j, pl.ds(0, qy, stride=2), :] + w1[j, pl.ds(1, qy, stride=2), :] for j in range(qx)], axis=0
    )
    tiles = qx * qy // 8
    total = None
    for t in range(tiles):
        source = iota((128, 128), 0) - left
        target = iota((128, 128), 1)
        inside = (source >= 0) & (source < hz)
        fold = jnp.where(inside & (target == t * qz + source // 2), 0.125, 0.0)
        part = dot(r[8 * t:8 * t + 8], fold)
        total = part if total is None else total + part
    pack[...] = total
    slots[mine] = total

    def gather(k):
        at = coords(k)
        d = number(at)
        return pltpu.make_async_remote_copy(
            src_ref=pack,
            dst_ref=slots.at[mine],
            send_sem=gather_sems.at[0, d],
            recv_sem=gather_sems.at[1, mine],
            device_id=at,
            device_id_type=MESH,
        )

    def gather_start(k, carry):
        gather(k).start()
        return carry

    others(gather_start)

    f1[c1:c1 + hx, PAD:PAD + hy, :] = e1[c1:c1 + hx, PAD:PAD + hy, :]
    xf1.start_x()
    xf0.wait_x()
    xf0.start_y()
    b2[...] = jnp.zeros_like(b2)
    b3[...] = jnp.zeros_like(b3)

    def gather_wait(k, carry):
        at = coords(k)
        d = number(at)
        copy = pltpu.make_async_remote_copy(
            src_ref=pack,
            dst_ref=slots.at[d],
            send_sem=gather_sems.at[0, d],
            recv_sem=gather_sems.at[1, d],
            device_id=at,
            device_id_type=MESH,
        )
        copy.wait_send()
        copy.wait_recv()
        return carry

    others(gather_wait)
    xf1.wait_x()
    xf1.start_y()
    per = 128 // qz

    def spread(c, carry):
        cx, cy = c // gy, lax.rem(c, gy)
        lane = iota((8, 128), 1)
        for g in range(gz // per):
            parts = [slots[c * gz + g * per + q] for q in range(per)]
            for t in range(tiles):
                p, h = t // (qy // 8), t % (qy // 8)
                tile = jnp.zeros((8, 128), jnp.float32)
                for q in range(per):
                    here = (lane >= q * qz) & (lane < (q + 1) * qz)
                    tile = jnp.where(here, pltpu.roll(parts[q], ((q - t) * qz) % 128, axis=1), tile)
                rows = pl.ds(pl.multiple_of(PAD + cy * qy + 8 * h, 8), 8)
                b2[1 + cx * qx + p, rows, 128 * g:128 * (g + 1)] = tile
        return carry

    lax.fori_loop(0, gx * gy, spread, 0)

    for step in range(4):
        update(v2, b2, t2, 1, 1 + x2, 1, step % 2, 16.0, True)

    def pair2(q, carry):
        r = residual(v2, b2, 1 + 2 * q, 16.0, True) + residual(v2, b2, 2 + 2 * q, 16.0, True)
        for g in range(z2 // 128):
            w2[g] = r[:, 128 * g:128 * (g + 1)]
        half = y2 // 2
        r = jnp.concatenate(
            [
                w2[g, pl.ds(PAD, half, stride=2), :] + w2[g, pl.ds(PAD + 1, half, stride=2), :]
                for g in range(z2 // 128)
            ],
            axis=1,
        )
        fold = jnp.where(iota((z2, z3p), 1) == iota((z2, z3p), 0) // 2, 0.125, 0.0)
        b3[1 + q, PAD:PAD + half, :] = dot(r, fold)
        return carry

    for q in range(x3):
        pair2(q, 0)
    xf0.wait_y()
    xf0.start_z()
    xf1.wait_y()
    xf1.start_z()

    def sweep3(k, planes):
        for colour in (0, 1):
            now = []
            for i in range(x3):
                total = beside(planes[i], True)
                if i > 0:
                    total = total + planes[i - 1]
                if i + 1 < x3:
                    total = total + planes[i + 1]
                value = (64.0 * b3[1 + i] + total) * SIXTH
                now.append(jnp.where(t3[...] == (i + colour) % 2, value, planes[i]))
            planes = tuple(now)
        return planes

    planes = lax.fori_loop(0, CSWEEPS, sweep3, tuple(v3[1 + i] for i in range(x3)))
    for i in range(x3):
        v3[1 + i] = planes[i]

    def lift3(q, carry):
        half = (y2 + 2 * PAD) // 2
        grow = jnp.where(iota((z3p, z2), 0) == iota((z3p, z2), 1) // 2, 1.0, 0.0)
        v = dot(v3[1 + q, PAD // 2:PAD // 2 + half, :], grow)
        for g in range(z2 // 128):
            w2[g, pl.ds(0, half, stride=2), :] = v[:, 128 * g:128 * (g + 1)]
            w2[g, pl.ds(1, half, stride=2), :] = v[:, 128 * g:128 * (g + 1)]
        for g in range(z2 // 128):
            lanes = slice(128 * g, 128 * (g + 1))
            for i in (1 + 2 * q, 2 + 2 * q):
                v2[i, :, lanes] = v2[i, :, lanes] + w2[g]
        return carry

    for q in range(x3):
        lift3(q, 0)

    for step in range(4):
        update(v2, b2, t2, 1, 1 + x2, 1, step % 2, 16.0, True)

    xf1.wait_z()
    rows1 = f1.shape[1]
    grow1 = jnp.where(
        iota((z2, 128), 0) == mz * qz + (iota((z2, 128), 1) - left + 2 * 128) // 2 - 128, 1.0, 0.0
    )
    rows2 = pl.ds(pl.multiple_of(my * qy, 8), rows1 // 2 + PAD)

    high2 = rows1 // 2 + PAD
    window = min(x2, qx + 2 * (SIDE1 // 2))
    begin = jnp.clip(mx * qx - SIDE1 // 2, 0, x2 - window)
    v = jnp.concatenate([v2[1 + begin + k, rows2, :] for k in range(window)], axis=0)
    v = dot(v, grow1)
    for k in range(window):
        part = v[k * high2:(k + 1) * high2]
        w1[k, pl.ds(0, high2, stride=2), :] = part
        w1[k, pl.ds(1, high2, stride=2), :] = part
    for k in range(window):
        i = c1 + 2 * (begin + k) - mx * hx
        lifted = w1[k, PAD:PAD + rows1, :]
        f1[i] = f1[i] + lifted
        f1[i + 1] = f1[i + 1] + lifted

    for step in range(4):
        first, last = span(c1, hx, 5 - step)
        update(f1, b1, t1, first, last, mx * hx + c1, step % 2, 4.0)

    xf0.wait_z()
    grow0 = jnp.where(
        iota((128, 256), 0) == (left + iota((128, 256), 1) // 2) % 128, 1.0, 0.0
    )
    half0 = rows0 // 2

    def lift1(c, carry):
        j = first + 2 * c
        v = jnp.concatenate([f1[j + k, PAD // 2:PAD // 2 + half0, :] for k in range(2)], axis=0)
        v = dot(v, grow0)
        for k in range(2):
            for g in range(2):
                at = pl.ds((2 * k + g) * rows0, half0, stride=2)
                w0[at, :] = v[k * half0:(k + 1) * half0, 128 * g:128 * (g + 1)]
                at = pl.ds((2 * k + g) * rows0 + 1, half0, stride=2)
                w0[at, :] = v[k * half0:(k + 1) * half0, 128 * g:128 * (g + 1)]
        for k in range(2):
            for g in range(2):
                lanes = slice(128 * g, 128 * (g + 1))
                lifted = w0[(2 * k + g) * rows0:(2 * k + g + 1) * rows0, :]
                for i in range(2):
                    at = c0 + 2 * (j + k - c1) + i
                    f0[at, :, lanes] = f0[at, :, lanes] + lifted
        return carry

    first, last = span(c1, hx, SIDE0 // 2)
    lax.fori_loop(0, (last - first) // 2, lift1, 0)

    for step in range(4):
        first, last = span(c0, lx, 3 - step)
        update(f0, b0, t0, first, last, mx * lx + c0, step % 2, 1.0)

    out_ref[...] = f0[c0:c0 + lx, PAD:PAD + ly, 0:128]


def local(sizes, right_side, start):
    gx, gy, gz = sizes
    lx, ly, lz = right_side.shape
    c0, c1 = DOWN0 + 1, SIDE1 + 2
    n0, n1 = lx + 2 * c0, lx // 2 + 2 * c1
    r0, r1 = ly + 2 * PAD, ly // 2 + 2 * PAD
    x2, y2, z2 = gx * lx // 4, gy * ly // 4, gz * lz // 4
    x3, y3, z3 = x2 // 2, y2 // 2, z2 // 2
    z3p = -(-z3 // 128) * 128
    f32, i32 = jnp.float32, jnp.int32
    count = gx * gy * gz
    return pl.pallas_call(
        functools.partial(kernel, sizes),
        out_shape=jax.ShapeDtypeStruct(start.shape, f32),
        in_specs=[pl.BlockSpec(memory_space=pltpu.VMEM)] * 2,
        out_specs=pl.BlockSpec(memory_space=pltpu.VMEM),
        scratch_shapes=[
            pltpu.VMEM((n0, r0, 256), f32),
            pltpu.VMEM((n0, r0, 256), f32),
            pltpu.VMEM((n0, r0, 256), f32),
            pltpu.VMEM((n1, r1, 128), f32),
            pltpu.VMEM((n1, r1, 128), f32),
            pltpu.VMEM((n1, r1, 128), f32),
            pltpu.VMEM((x2 + 2, y2 + 2 * PAD, z2), f32),
            pltpu.VMEM((x2 + 2, y2 + 2 * PAD, z2), f32),
            pltpu.VMEM((x3 + 2, y3 + 2 * PAD, z3p), f32),
            pltpu.VMEM((x3 + 2, y3 + 2 * PAD, z3p), f32),
            pltpu.VMEM((r0, 256), i32),
            pltpu.VMEM((r1, 128), i32),
            pltpu.VMEM((y2 + 2 * PAD, z2), i32),
            pltpu.VMEM((y3 + 2 * PAD, z3p), i32),
            pltpu.VMEM((max(lx // 2 * ly, 4 * r0), 128), f32),
            pltpu.VMEM((lx // 4 + SIDE1, r1 + 2 * PAD, 128), f32),
            pltpu.VMEM((z2 // 128, y2 + 2 * PAD, 128), f32),
            pltpu.VMEM((8, 128), f32),
            pltpu.VMEM((count, 8, 128), f32),
            pltpu.VMEM((2, 2, r0, 128), f32),
            pltpu.VMEM((2, 2, r0, 128), f32),
            pltpu.VMEM((2, 2, r0, 128), f32),
            pltpu.VMEM((2, 2, r1, 128), f32),
            pltpu.VMEM((2, 2, r1, 128), f32),
            pltpu.SemaphoreType.DMA((5, 2, 8)),
            pltpu.SemaphoreType.DMA((2, count)),
        ],
        compiler_params=pltpu.CompilerParams(
            collective_id=0, has_side_effects=True, vmem_limit_bytes=60 * 1024 * 1024
        ),
    )(right_side, start)


def solution(mesh):
    sizes = (mesh.shape["gx"], mesh.shape["gy"], mesh.shape["gz"])
    spec = P("gx", "gy", "gz")
    return jax.shard_map(
        functools.partial(local, sizes), mesh=mesh, in_specs=(spec, spec), out_specs=spec, check_vma=False
    )
```

```python
import functools

import jax
import jax.numpy as jnp
from jax import lax
from jax.experimental import pallas as pl
from jax.experimental.pallas import tpu as pltpu
from jax.sharding import PartitionSpec as P

MESH = pl.DeviceIdType.MESH
SIXTH = 1.0 / 6.0
PAD = 8
TOP = 16
DOWN0 = 5
SIDE0 = 4
SIDE1 = 6
RHS1 = 5
CSWEEPS = 8
CHUNK0 = 2
CHUNK1 = 4


def dot(a, b):
    return jnp.dot(a, b, precision=lax.Precision.HIGHEST, preferred_element_type=jnp.float32)


def iota(shape, axis):
    return lax.broadcasted_iota(jnp.int32, shape, axis)


def beside(v, edge):
    rows, lanes = v.shape
    up = pltpu.roll(v, 1, axis=0) + pltpu.roll(v, rows - 1, axis=0)
    low = pltpu.roll(v, 1, axis=1)
    high = pltpu.roll(v, lanes - 1, axis=1)
    if edge:
        lane = iota(v.shape, 1)
        low = jnp.where(lane == 0, 0.0, low)
        high = jnp.where(lane == lanes - 1, 0.0, high)
    return up + (low + high)


def update(v_ref, b_ref, code, first, last, origin, colour, factor, edge=False, chunk=4):
    def some(start, size):
        planes = [v_ref[start - 1 + k] for k in range(size + 2)]
        sides = [beside(planes[k + 1], edge) for k in range(size)]
        fresh = []
        for k in range(size):
            total = (planes[k] + planes[k + 2]) + sides[k]
            want = lax.rem(start + (k + origin + colour), 2)
            value = (factor * b_ref[start + k] + total) * SIXTH
            fresh.append(jnp.where(code[...] == want, value, planes[k + 1]))
        for k in range(size):
            v_ref[start + k] = fresh[k]

    if isinstance(first, int) and last - first <= chunk:
        some(first, last - first)
        return

    def body(c, carry):
        some(jnp.minimum(first + c * chunk, last - chunk), chunk)
        return carry

    lax.fori_loop(0, (last - first + chunk - 1) // chunk, body, 0)


def residual(v_ref, b_ref, i, factor, edge=False):
    v = v_ref[i]
    total = (v_ref[i - 1] + v_ref[i + 1]) + beside(v, edge)
    return b_ref[i] - (6.0 * v - total) * (1.0 / factor)


def turned(tiles, shift, edge_lane):
    moved = [pltpu.roll(tile, shift, axis=1) for tile in tiles]
    if len(moved) == 1:
        return moved
    lane = iota(tiles[0].shape, 1)
    return [jnp.where(lane == edge_lane, moved[1], moved[0]), jnp.where(lane == edge_lane, moved[0], moved[1])]


def fine_update(v_ref, b_ref, code, first, last, origin, colour, factor, chunk):
    tiles, rows = v_ref.shape[1], v_ref.shape[2] - 2 * PAD

    def some(start, size):
        planes = [[v_ref[start - 1 + k, g, PAD:PAD + rows] for g in range(tiles)] for k in range(size + 2)]
        fresh = []
        for k in range(1, size + 1):
            i = start + (k - 1)
            low = turned(planes[k], 1, 0)
            high = turned(planes[k], 127, 127)
            want = lax.rem(start + (k - 1 + origin + colour), 2)
            for g in range(tiles):
                total = v_ref[i, g, PAD - 1:PAD - 1 + rows] + v_ref[i, g, PAD + 1:PAD + 1 + rows]
                total = (total + (planes[k - 1][g] + planes[k + 1][g])) + (low[g] + high[g])
                value = (factor * b_ref[i, g, PAD:PAD + rows] + total) * SIXTH
                fresh.append((i, g, jnp.where(code[g] == want, value, planes[k][g])))
        for i, g, value in fresh:
            v_ref[i, g, PAD:PAD + rows] = value

    def body(c, carry):
        some(jnp.minimum(first + c * chunk, last - chunk), chunk)
        return carry

    lax.fori_loop(0, (last - first + chunk - 1) // chunk, body, 0)


def fine_residual(v_ref, b_ref, i, rows, factor):
    own = slice(TOP, TOP + rows)
    tiles = [v_ref[i, g, own] for g in range(v_ref.shape[1])]
    total = v_ref[i, 0, TOP - 1:TOP - 1 + rows] + v_ref[i, 0, TOP + 1:TOP + 1 + rows]
    total = total + (v_ref[i - 1, 0, own] + v_ref[i + 1, 0, own])
    total = total + (turned(tiles, 1, 0)[0] + turned(tiles, 127, 127)[0])
    return b_ref[i, 0, own] - (6.0 * tiles[0] - total) * (1.0 / factor)


class Exchange:
    def __init__(self, ref, sems, send, recv, box, depth, me, sizes):
        self.ref, self.sems, self.send, self.recv = ref, sems, send, recv
        self.c0, self.n, self.rows, self.l0, self.lanes = box
        self.depth, self.me, self.sizes = depth, me, sizes

    def _x(self):
        c0, n, depth = self.c0, self.n, self.depth
        gx = self.sizes[0]
        mx, my, mz = self.me
        rows = pl.ds(TOP, self.rows)
        out = []
        hop = 1
        slot = 0
        while (hop - 1) * n < depth and hop < gx:
            count = min(n, depth - (hop - 1) * n)
            far = (hop - 1) * n
            up = (c0 + n - count, c0 - far - count, mx + hop < gx, mx + hop, mx >= hop)
            down = (c0, c0 + n + far, mx >= hop, mx - hop, mx + hop < gx)
            for src, dst, may_send, peer, may_recv in (up, down):
                copy = pltpu.make_async_remote_copy(
                    src_ref=self.ref.at[pl.ds(src, count), 0, rows],
                    dst_ref=self.ref.at[pl.ds(dst, count), 0, rows],
                    send_sem=self.sems.at[0, slot],
                    recv_sem=self.sems.at[1, slot],
                    device_id=(peer, my, mz),
                    device_id_type=MESH,
                )
                out.append((copy, may_send, may_recv))
                slot += 1
            hop += 1
        return out

    def _y(self):
        gy = self.sizes[1]
        mx, my, mz = self.me
        planes = pl.ds(self.c0 - self.depth, self.n + 2 * self.depth)
        out = []
        up = (TOP + self.rows - PAD, TOP - PAD, my + 1 < gy, my + 1, my >= 1)
        down = (TOP, TOP + self.rows, my >= 1, my - 1, my + 1 < gy)
        for k, (src, dst, may_send, peer, may_recv) in enumerate((up, down)):
            copy = pltpu.make_async_remote_copy(
                src_ref=self.ref.at[planes, 0, pl.ds(src, PAD)],
                dst_ref=self.ref.at[planes, 0, pl.ds(dst, PAD)],
                send_sem=self.sems.at[0, 4 + k],
                recv_sem=self.sems.at[1, 4 + k],
                device_id=(mx, peer, mz),
                device_id_type=MESH,
            )
            out.append((copy, may_send, may_recv))
        return out

    def _z(self):
        gz = self.sizes[2]
        mx, my, mz = self.me
        out = []
        up = (0, mz + 1 < gz, mz + 1, mz >= 1)
        down = (1, mz >= 1, mz - 1, mz + 1 < gz)
        for k, may_send, peer, may_recv in (up, down):
            copy = pltpu.make_async_remote_copy(
                src_ref=self.send.at[k],
                dst_ref=self.recv.at[k],
                send_sem=self.sems.at[0, 6 + k],
                recv_sem=self.sems.at[1, 6 + k],
                device_id=(mx, my, peer),
                device_id_type=MESH,
            )
            out.append((copy, may_send, may_recv))
        return out

    def _start(self, copies):
        for copy, may_send, may_recv in copies:
            pl.when(may_send)(copy.start)

    def _wait(self, copies):
        for copy, may_send, may_recv in copies:
            pl.when(may_send)(copy.wait_send)
            pl.when(may_recv)(copy.wait_recv)

    def start_x(self):
        self._start(self._x())

    def wait_x(self):
        self._wait(self._x())

    def start_y(self):
        self._start(self._y())

    def wait_y(self):
        self._wait(self._y())

    def _planes(self):
        return range(self.c0 - self.depth, self.c0 + self.n + self.depth)

    def start_z(self):
        d = self.depth
        shape = self.send.shape[1:]
        lane = iota(shape, 1)
        up = jnp.zeros(shape, jnp.float32)
        down = jnp.zeros(shape, jnp.float32)
        for k, i in enumerate(self._planes()):
            v = self.ref[i, 0, PAD:PAD + shape[0]]
            here = (lane >= k * d) & (lane < k * d + d)
            up = jnp.where(here, pltpu.roll(v, (k * d - (self.l0 + self.lanes - d)) % 128, axis=1), up)
            down = jnp.where(here, pltpu.roll(v, (k * d - self.l0) % 128, axis=1), down)
        self.send[0] = up
        self.send[1] = down
        self._start(self._z())

    def wait_z(self):
        self._wait(self._z())
        d = self.depth
        gz = self.sizes[2]
        mz = self.me[2]
        shape = self.recv.shape[1:]
        lane = iota(shape, 1)
        low_at = (self.l0 - d) % 128
        high_at = (self.l0 + self.lanes) % 128
        is_low = (lane >= low_at) & (lane < low_at + d)
        is_high = (lane >= high_at) & (lane < high_at + d)
        low_buffer = jnp.where(mz >= 1, self.recv[0], 0.0)
        high_buffer = jnp.where(mz + 1 < gz, self.recv[1], 0.0)
        whole = self.ref.shape[1] == 2
        rows = slice(PAD, PAD + shape[0])
        for k, i in enumerate(self._planes()):
            low = pltpu.roll(low_buffer, (low_at - k * d) % 128, axis=1)
            high = pltpu.roll(high_buffer, (high_at - k * d) % 128, axis=1)
            if whole:
                self.ref[i, 1, rows] = jnp.where(is_low, low, jnp.where(is_high, high, 0.0))
            else:
                v = self.ref[i, 0, rows]
                self.ref[i, 0, rows] = jnp.where(is_low, low, jnp.where(is_high, high, v))


def kernel(
    sizes, rhs_ref, start_ref, out_ref,
    e0, b0, f0, e1, b1, f1, v2, b2, v3, b3,
    t0, t1, t2, t3, w0, w1, w2, pack, slots, side_send, side_recv,
    za, zb, zc, zd, ze, halo_sems, gather_sems,
):
    gx, gy, gz = sizes
    count = gx * gy * gz
    me = mx, my, mz = lax.axis_index("gx"), lax.axis_index("gy"), lax.axis_index("gz")
    mine = (mx * gy + my) * gz + mz
    lx, ly, lz = rhs_ref.shape
    c0, c1 = DOWN0 + 1, SIDE1 + 2
    hx, hy, hz = lx // 2, ly // 2, lz // 2
    qx, qy, qz = hx // 2, hy // 2, hz // 2
    x2, y2, z2 = gx * qx, gy * qy, gz * qz
    x3, y3, z3 = x2 // 2, y2 // 2, z2 // 2
    z3p = v3.shape[2]
    left = (128 - hz) // 2

    def coords(k):
        steps = (k // (gy * gz), k // gz % gy, k % gz)
        moved = [at + step for at, step in zip(me, steps)]
        return tuple(jnp.where(at >= size, at - size, at) for at, size in zip(moved, sizes))

    def number(at):
        return (at[0] * gy + at[1]) * gz + at[2]

    def others(body):
        if count <= 64:
            for k in range(1, count):
                body(k, 0)
        else:
            lax.fori_loop(1, count, body, 0)

    for ref in (e1, b1, f1, v2, v3):
        ref[...] = jnp.zeros_like(ref)
    for ref in (e0, b0, f0):
        n0 = ref.shape[0]
        ref[:, :, 0:TOP] = jnp.zeros((n0, 2, TOP, 128), jnp.float32)
        ref[:, :, TOP + ly:] = jnp.zeros((n0, 2, TOP, 128), jnp.float32)
        for i in list(range(c0)) + list(range(c0 + lx, n0)):
            ref[i] = jnp.zeros(ref.shape[1:], jnp.float32)

    barrier = pltpu.get_barrier_semaphore()

    def greet(k, carry):
        pl.semaphore_signal(barrier, inc=1, device_id=coords(k), device_id_type=MESH)
        return carry

    others(greet)

    e0[c0:c0 + lx, 0, TOP:TOP + ly] = start_ref[...]
    b0[c0:c0 + lx, 0, TOP:TOP + ly] = rhs_ref[...]

    def code(shape, row0, lane_of, bounds):
        y = iota(shape, 0) + row0
        z = lane_of(iota(shape, 1))
        inside = (y >= 0) & (y < bounds[0]) & (z >= 0) & (z < bounds[1])
        return jnp.where(inside, (y + z) & 1, 5)

    fine = (gy * ly, gz * lz)
    t0[0] = code(t0.shape[1:], my * ly - PAD, lambda c: mz * lz + c, fine)
    t0[1] = code(t0.shape[1:], my * ly - PAD, lambda c: mz * lz + jnp.where(c < 64, c + 128, c - 128), fine)
    t1[0] = code(t1.shape[1:], my * hy - PAD, lambda c: mz * hz + c - left, (gy * hy, gz * hz))
    t2[...] = code(t2.shape, -PAD, lambda c: c, (y2, z2))
    t3[...] = code(t3.shape, -PAD, lambda c: c, (y3, z3))

    pl.semaphore_wait(barrier, count - 1)

    box0 = (c0, lx, ly, 0, lz)
    box1 = (c1, hx, hy, left, hz)
    xe0 = Exchange(e0, halo_sems.at[0], za.at[0], za.at[1], box0, DOWN0, me, sizes)
    xb0 = Exchange(b0, halo_sems.at[1], zb.at[0], zb.at[1], box0, DOWN0 - 1, me, sizes)
    xf0 = Exchange(f0, halo_sems.at[2], zc.at[0], zc.at[1], box0, SIDE0, me, sizes)
    xb1 = Exchange(b1, halo_sems.at[3], zd.at[0], zd.at[1], box1, RHS1, me, sizes)
    xf1 = Exchange(f1, halo_sems.at[4], ze.at[0], ze.at[1], box1, SIDE1, me, sizes)

    def outer(direction, k):
        return c0 + lx - k if direction == 0 else c0 + k - 1

    def halo(direction, k):
        return c0 - k if direction == 0 else c0 + lx + k - 1

    own = slice(TOP, TOP + ly)
    checks = t0[0, PAD:PAD + ly]

    def black(i):
        return checks == lax.rem(mx * lx + (i + c0 + 1), 2)

    def merged(ref, direction, k):
        i = outer(direction, k)
        return jnp.where(black(i), ref[i, 0, own], ref[outer(direction, k + 1), 0, own])

    peers = ((mx + 1 < gx, mx + 1, mx >= 1), (mx >= 1, mx - 1, mx + 1 < gx))

    def side_copies(planes, group):
        return [
            (
                pltpu.make_async_remote_copy(
                    src_ref=side_send.at[d, planes],
                    dst_ref=side_recv.at[d, planes],
                    send_sem=halo_sems.at[group, 0, d],
                    recv_sem=halo_sems.at[group, 1, d],
                    device_id=(peer, my, mz),
                    device_id_type=MESH,
                ),
                may_send,
                may_recv,
            )
            for d, (may_send, peer, may_recv) in enumerate(peers)
        ]

    near = DOWN0 - 2
    rhs_copies = [
        (
            pltpu.make_async_remote_copy(
                src_ref=rhs_ref.at[pl.ds((lx - near, 0)[d], near)],
                dst_ref=b0.at[pl.ds((c0 - near, c0 + lx)[d], near), 0, pl.ds(TOP, ly)],
                send_sem=halo_sems.at[1, 0, d],
                recv_sem=halo_sems.at[1, 1, d],
                device_id=(peer, my, mz),
                device_id_type=MESH,
            ),
            may_send,
            may_recv,
        )
        for d, (may_send, peer, may_recv) in enumerate(peers)
    ]
    for copy, may_send, may_recv in rhs_copies:
        pl.when(may_send)(copy.start)
    for d in range(2):
        side_send[d, 0] = merged(e0, d, 1)
        side_send[d, 1] = merged(e0, d, 3)
        i = outer(d, 5)
        moved = pltpu.roll(b0[outer(d, 4), 0, own], 1, axis=0)
        side_send[d, 2] = jnp.where(black(i), e0[i, 0, own], moved)
    start_copies = side_copies(pl.ds(0, 3), 0)
    xe0._start(start_copies)
    xe0._wait(start_copies)
    for d in range(2):

        @pl.when(peers[d][2])
        def _():
            for k in range(1, 5):
                e0[halo(d, k), 0, own] = side_recv[d, (k - 1) // 2]
            e0[halo(d, 5), 0, own] = side_recv[d, 2]
            b0[halo(d, 4), 0, own] = pltpu.roll(side_recv[d, 2], ly - 1, axis=0)

    xe0.start_y()
    xb0._wait(rhs_copies)
    xb0.start_y()
    xe0.wait_y()
    xe0.start_z()
    xb0.wait_y()
    xb0.start_z()
    xe0.wait_z()
    xb0.wait_z()

    def span(c, n, depth):
        return (
            jnp.maximum(c - depth, c - mx * n),
            jnp.minimum(c + n + depth, c + (gx - mx) * n),
        )

    for step in range(4):
        first, last = span(c0, lx, 4 - step)
        fine_update(e0, b0, t0, first, last, mx * lx + c0, step % 2, 1.0, CHUNK0)

    def pair0(j, carry):
        i = c0 + 2 * j
        r = fine_residual(e0, b0, i, ly, 1.0) + fine_residual(e0, b0, i + 1, ly, 1.0)
        w0[j * ly:(j + 1) * ly, :] = r
        return carry

    for j in range(hx):
        pair0(j, 0)
    r = w0[pl.ds(0, hx * hy, stride=2), :] + w0[pl.ds(1, hx * hy, stride=2), :]
    fold = jnp.where(iota((128, 128), 1) == left + iota((128, 128), 0) // 2, 0.125, 0.0)
    r = dot(r, fold)
    for j in range(hx):
        b1[c1 + j, 0, TOP:TOP + hy] = r[j * hy:(j + 1) * hy]

    xb1.start_x()
    f0[c0:c0 + lx, 0, own] = e0[c0:c0 + lx, 0, own]
    for d in range(2):
        side_send[d, 3] = merged(f0, d, 1)
        side_send[d, 4] = merged(f0, d, 3)
    side0 = side_copies(pl.ds(3, 2), 2)
    xb1.wait_x()
    xb1.start_y()
    xb1.wait_y()
    xb1.start_z()
    xb1.wait_z()

    for step in range(4):
        first, last = span(c1, hx, 4 - step)
        fine_update(e1, b1, t1, first, last, mx * hx + c1, step % 2, 4.0, CHUNK1)

    for j in range(qx):
        i = c1 + 2 * j
        w1[j, 0:hy, :] = fine_residual(e1, b1, i, hy, 4.0) + fine_residual(e1, b1, i + 1, hy, 4.0)
    r = jnp.concatenate(
        [w1[j, pl.ds(0, qy, stride=2), :] + w1[j, pl.ds(1, qy, stride=2), :] for j in range(qx)], axis=0
    )
    tiles = qx * qy // 8
    total = None
    for t in range(tiles):
        source = iota((128, 128), 0) - left
        target = iota((128, 128), 1)
        inside = (source >= 0) & (source < hz)
        fold = jnp.where(inside & (target == t * qz + source // 2), 0.125, 0.0)
        part = dot(r[8 * t:8 * t + 8], fold)
        total = part if total is None else total + part
    pack[...] = total
    slots[mine] = total

    def gather(k):
        at = coords(k)
        d = number(at)
        return pltpu.make_async_remote_copy(
            src_ref=pack,
            dst_ref=slots.at[mine],
            send_sem=gather_sems.at[0, d],
            recv_sem=gather_sems.at[1, mine],
            device_id=at,
            device_id_type=MESH,
        )

    def gather_start(k, carry):
        gather(k).start()
        return carry

    others(gather_start)

    f1[c1:c1 + hx, 0, TOP:TOP + hy] = e1[c1:c1 + hx, 0, TOP:TOP + hy]
    xf1.start_x()
    xf0._start(side0)
    b2[...] = jnp.zeros_like(b2)
    b3[...] = jnp.zeros_like(b3)

    def gather_wait(k, carry):
        at = coords(k)
        d = number(at)
        copy = pltpu.make_async_remote_copy(
            src_ref=pack,
            dst_ref=slots.at[d],
            send_sem=gather_sems.at[0, d],
            recv_sem=gather_sems.at[1, d],
            device_id=at,
            device_id_type=MESH,
        )
        copy.wait_send()
        copy.wait_recv()
        return carry

    others(gather_wait)
    xf1.wait_x()
    xf1.start_y()
    xf0._wait(side0)
    for d in range(2):

        @pl.when(peers[d][2])
        def _():
            for k in range(1, 5):
                f0[halo(d, k), 0, own] = side_recv[d, 3 + (k - 1) // 2]

    xf0.start_y()
    per = 128 // qz

    def spread(c, carry):
        cx, cy = c // gy, lax.rem(c, gy)
        lane = iota((8, 128), 1)
        for g in range(gz // per):
            parts = [slots[c * gz + g * per + q] for q in range(per)]
            for t in range(tiles):
                p, h = t // (qy // 8), t % (qy // 8)
                tile = jnp.zeros((8, 128), jnp.float32)
                for q in range(per):
                    here = (lane >= q * qz) & (lane < (q + 1) * qz)
                    tile = jnp.where(here, pltpu.roll(parts[q], ((q - t) * qz) % 128, axis=1), tile)
                rows = pl.ds(pl.multiple_of(PAD + cy * qy + 8 * h, 8), 8)
                b2[1 + cx * qx + p, rows, 128 * g:128 * (g + 1)] = tile
        return carry

    lax.fori_loop(0, gx * gy, spread, 0)

    for step in range(4):
        update(v2, b2, t2, 1, 1 + x2, 1, step % 2, 16.0, True)

    def pair2(q, carry):
        r = residual(v2, b2, 1 + 2 * q, 16.0, True) + residual(v2, b2, 2 + 2 * q, 16.0, True)
        for g in range(z2 // 128):
            w2[g] = r[:, 128 * g:128 * (g + 1)]
        half = y2 // 2
        r = jnp.concatenate(
            [
                w2[g, pl.ds(PAD, half, stride=2), :] + w2[g, pl.ds(PAD + 1, half, stride=2), :]
                for g in range(z2 // 128)
            ],
            axis=1,
        )
        fold = jnp.where(iota((z2, z3p), 1) == iota((z2, z3p), 0) // 2, 0.125, 0.0)
        b3[1 + q, PAD:PAD + half, :] = dot(r, fold)
        return carry

    for q in range(x3):
        pair2(q, 0)
    xf0.wait_y()
    xf0.start_z()
    xf1.wait_y()
    xf1.start_z()

    def sweep3(k, planes):
        for colour in (0, 1):
            now = []
            for i in range(x3):
                total = beside(planes[i], True)
                if i > 0:
                    total = total + planes[i - 1]
                if i + 1 < x3:
                    total = total + planes[i + 1]
                value = (64.0 * b3[1 + i] + total) * SIXTH
                now.append(jnp.where(t3[...] == (i + colour) % 2, value, planes[i]))
            planes = tuple(now)
        return planes

    planes = lax.fori_loop(0, CSWEEPS, sweep3, tuple(v3[1 + i] for i in range(x3)))
    for i in range(x3):
        v3[1 + i] = planes[i]

    def lift3(q, carry):
        half = (y2 + 2 * PAD) // 2
        grow = jnp.where(iota((z3p, z2), 0) == iota((z3p, z2), 1) // 2, 1.0, 0.0)
        v = dot(v3[1 + q, PAD // 2:PAD // 2 + half, :], grow)
        for g in range(z2 // 128):
            w2[g, pl.ds(0, half, stride=2), :] = v[:, 128 * g:128 * (g + 1)]
            w2[g, pl.ds(1, half, stride=2), :] = v[:, 128 * g:128 * (g + 1)]
        for g in range(z2 // 128):
            lanes = slice(128 * g, 128 * (g + 1))
            for i in (1 + 2 * q, 2 + 2 * q):
                v2[i, :, lanes] = v2[i, :, lanes] + w2[g]
        return carry

    for q in range(x3):
        lift3(q, 0)

    for step in range(4):
        update(v2, b2, t2, 1, 1 + x2, 1, step % 2, 16.0, True)

    xf1.wait_z()
    rows1 = f1.shape[2]
    grow1 = jnp.where(
        iota((z2, 128), 0) == mz * qz + (iota((z2, 128), 1) - left + 2 * 128) // 2 - 128, 1.0, 0.0
    )
    rows2 = pl.ds(pl.multiple_of(my * qy, 8), rows1 // 2)

    high2 = rows1 // 2
    window = min(x2, qx + 2 * (SIDE1 // 2))
    begin = jnp.clip(mx * qx - SIDE1 // 2, 0, x2 - window)
    v = jnp.concatenate([v2[1 + begin + k, rows2, :] for k in range(window)], axis=0)
    v = dot(v, grow1)
    for k in range(window):
        part = v[k * high2:(k + 1) * high2]
        w1[k, pl.ds(0, high2, stride=2), :] = part
        w1[k, pl.ds(1, high2, stride=2), :] = part
    for k in range(window):
        i = c1 + 2 * (begin + k) - mx * hx
        rows = slice(PAD, rows1 - PAD)
        lifted = w1[k, rows, :]
        f1[i, 0, rows] = f1[i, 0, rows] + lifted
        f1[i + 1, 0, rows] = f1[i + 1, 0, rows] + lifted

    for step in range(4):
        first, last = span(c1, hx, 5 - step)
        fine_update(f1, b1, t1, first, last, mx * hx + c1, step % 2, 4.0, CHUNK1)

    xf0.wait_z()
    grow0 = jnp.where(
        iota((128, 256), 0) == (left + iota((128, 256), 1) // 2) % 128, 1.0, 0.0
    )
    rows0 = f0.shape[2]
    half0 = rows0 // 2

    def lift1(c, carry):
        j = first + 2 * c
        v = jnp.concatenate([f1[j + k, 0, PAD:PAD + half0] for k in range(2)], axis=0)
        v = dot(v, grow0)
        for k in range(2):
            for g in range(2):
                at = pl.ds((2 * k + g) * rows0, half0, stride=2)
                w0[at, :] = v[k * half0:(k + 1) * half0, 128 * g:128 * (g + 1)]
                at = pl.ds((2 * k + g) * rows0 + 1, half0, stride=2)
                w0[at, :] = v[k * half0:(k + 1) * half0, 128 * g:128 * (g + 1)]
        for k in range(2):
            for g in range(2):
                rows = slice(PAD, rows0 - PAD)
                base = (2 * k + g) * rows0
                lifted = w0[base + PAD:base + rows0 - PAD, :]
                for i in range(2):
                    at = c0 + 2 * (j + k - c1) + i
                    f0[at, g, rows] = f0[at, g, rows] + lifted
        return carry

    first, last = span(c1, hx, SIDE0 // 2)
    lax.fori_loop(0, (last - first) // 2, lift1, 0)

    for step in range(4):
        first, last = span(c0, lx, 3 - step)
        fine_update(f0, b0, t0, first, last, mx * lx + c0, step % 2, 1.0, CHUNK0)

    out_ref[...] = f0[c0:c0 + lx, 0, own]


def local(sizes, right_side, start):
    gx, gy, gz = sizes
    lx, ly, lz = right_side.shape
    c0, c1 = DOWN0 + 1, SIDE1 + 2
    n0, n1 = lx + 2 * c0, lx // 2 + 2 * c1
    r0, r1 = ly + 2 * TOP, ly // 2 + 2 * TOP
    x2, y2, z2 = gx * lx // 4, gy * ly // 4, gz * lz // 4
    x3, y3, z3 = x2 // 2, y2 // 2, z2 // 2
    z3p = -(-z3 // 128) * 128
    f32, i32 = jnp.float32, jnp.int32
    count = gx * gy * gz
    return pl.pallas_call(
        functools.partial(kernel, sizes),
        out_shape=jax.ShapeDtypeStruct(start.shape, f32),
        in_specs=[pl.BlockSpec(memory_space=pltpu.VMEM)] * 2,
        out_specs=pl.BlockSpec(memory_space=pltpu.VMEM),
        scratch_shapes=[
            pltpu.VMEM((n0, 2, r0, 128), f32),
            pltpu.VMEM((n0, 2, r0, 128), f32),
            pltpu.VMEM((n0, 2, r0, 128), f32),
            pltpu.VMEM((n1, 1, r1, 128), f32),
            pltpu.VMEM((n1, 1, r1, 128), f32),
            pltpu.VMEM((n1, 1, r1, 128), f32),
            pltpu.VMEM((x2 + 2, y2 + 2 * PAD, z2), f32),
            pltpu.VMEM((x2 + 2, y2 + 2 * PAD, z2), f32),
            pltpu.VMEM((x3 + 2, y3 + 2 * PAD, z3p), f32),
            pltpu.VMEM((x3 + 2, y3 + 2 * PAD, z3p), f32),
            pltpu.VMEM((2, r0 - 2 * PAD, 128), i32),
            pltpu.VMEM((1, r1 - 2 * PAD, 128), i32),
            pltpu.VMEM((y2 + 2 * PAD, z2), i32),
            pltpu.VMEM((y3 + 2 * PAD, z3p), i32),
            pltpu.VMEM((max(lx // 2 * ly, 4 * r0), 128), f32),
            pltpu.VMEM((lx // 4 + SIDE1, r1, 128), f32),
            pltpu.VMEM((z2 // 128, y2 + 2 * PAD, 128), f32),
            pltpu.VMEM((8, 128), f32),
            pltpu.VMEM((count, 8, 128), f32),
            pltpu.VMEM((2, 5, ly, 128), f32),
            pltpu.VMEM((2, 5, ly, 128), f32),
            pltpu.VMEM((2, 2, r0 - 2 * PAD, 128), f32),
            pltpu.VMEM((2, 2, r0 - 2 * PAD, 128), f32),
            pltpu.VMEM((2, 2, r0 - 2 * PAD, 128), f32),
            pltpu.VMEM((2, 2, r1 - 2 * PAD, 128), f32),
            pltpu.VMEM((2, 2, r1 - 2 * PAD, 128), f32),
            pltpu.SemaphoreType.DMA((5, 2, 8)),
            pltpu.SemaphoreType.DMA((2, count)),
        ],
        compiler_params=pltpu.CompilerParams(
            collective_id=0, has_side_effects=True, vmem_limit_bytes=60 * 1024 * 1024
        ),
    )(right_side, start)


def solution(mesh):
    sizes = (mesh.shape["gx"], mesh.shape["gy"], mesh.shape["gz"])
    spec = P("gx", "gy", "gz")
    return jax.shard_map(
        functools.partial(local, sizes), mesh=mesh, in_specs=(spec, spec), out_specs=spec, check_vma=False
    )
```

```python
import functools

import jax
import jax.numpy as jnp
from jax import lax
from jax.experimental import pallas as pl
from jax.experimental.pallas import tpu as pltpu
from jax.sharding import PartitionSpec as P

MESH = pl.DeviceIdType.MESH
SIXTH = 1.0 / 6.0
PAD = 8
TOP = 16
DOWN0 = 5
SIDE0 = 4
SIDE1 = 6
RHS1 = 5
CSWEEPS = 8
CHUNK0 = 2
CHUNK1 = 4


def dot(a, b):
    return jnp.dot(a, b, precision=lax.Precision.HIGHEST, preferred_element_type=jnp.float32)


def iota(shape, axis):
    return lax.broadcasted_iota(jnp.int32, shape, axis)


def beside(v, edge):
    rows, lanes = v.shape
    up = pltpu.roll(v, 1, axis=0) + pltpu.roll(v, rows - 1, axis=0)
    low = pltpu.roll(v, 1, axis=1)
    high = pltpu.roll(v, lanes - 1, axis=1)
    if edge:
        lane = iota(v.shape, 1)
        low = jnp.where(lane == 0, 0.0, low)
        high = jnp.where(lane == lanes - 1, 0.0, high)
    return up + (low + high)


def update(v_ref, b_ref, code, first, last, origin, colour, factor, edge=False, chunk=4):
    def some(start, size):
        planes = [v_ref[start - 1 + k] for k in range(size + 2)]
        sides = [beside(planes[k + 1], edge) for k in range(size)]
        fresh = []
        for k in range(size):
            total = (planes[k] + planes[k + 2]) + sides[k]
            want = lax.rem(start + (k + origin + colour), 2)
            value = (factor * b_ref[start + k] + total) * SIXTH
            fresh.append(jnp.where(code[...] == want, value, planes[k + 1]))
        for k in range(size):
            v_ref[start + k] = fresh[k]

    if isinstance(first, int) and last - first <= chunk:
        some(first, last - first)
        return

    def body(c, carry):
        some(jnp.minimum(first + c * chunk, last - chunk), chunk)
        return carry

    lax.fori_loop(0, (last - first + chunk - 1) // chunk, body, 0)


def residual(v_ref, b_ref, i, factor, edge=False):
    v = v_ref[i]
    total = (v_ref[i - 1] + v_ref[i + 1]) + beside(v, edge)
    return b_ref[i] - (6.0 * v - total) * (1.0 / factor)


def turned(tiles, shift, edge_lane):
    moved = [pltpu.roll(tile, shift, axis=1) for tile in tiles]
    if len(moved) == 1:
        return moved
    lane = iota(tiles[0].shape, 1)
    return [jnp.where(lane == edge_lane, moved[1], moved[0]), jnp.where(lane == edge_lane, moved[0], moved[1])]


def fine_update(v_ref, b_ref, code, first, last, origin, colour, factor, chunk):
    tiles, rows = v_ref.shape[1], v_ref.shape[2] - 2 * PAD

    def some(start, size):
        planes = [[v_ref[start - 1 + k, g, PAD:PAD + rows] for g in range(tiles)] for k in range(size + 2)]
        fresh = []
        for k in range(1, size + 1):
            i = start + (k - 1)
            low = turned(planes[k], 1, 0)
            high = turned(planes[k], 127, 127)
            want = lax.rem(start + (k - 1 + origin + colour), 2)
            for g in range(tiles):
                total = v_ref[i, g, PAD - 1:PAD - 1 + rows] + v_ref[i, g, PAD + 1:PAD + 1 + rows]
                total = (total + (planes[k - 1][g] + planes[k + 1][g])) + (low[g] + high[g])
                value = (factor * b_ref[i, g, PAD:PAD + rows] + total) * SIXTH
                fresh.append((i, g, jnp.where(code[g] == want, value, planes[k][g])))
        for i, g, value in fresh:
            v_ref[i, g, PAD:PAD + rows] = value

    def body(c, carry):
        some(jnp.minimum(first + c * chunk, last - chunk), chunk)
        return carry

    lax.fori_loop(0, (last - first + chunk - 1) // chunk, body, 0)


def fine_residual(v_ref, b_ref, i, rows, factor):
    own = slice(TOP, TOP + rows)
    tiles = [v_ref[i, g, own] for g in range(v_ref.shape[1])]
    total = v_ref[i, 0, TOP - 1:TOP - 1 + rows] + v_ref[i, 0, TOP + 1:TOP + 1 + rows]
    total = total + (v_ref[i - 1, 0, own] + v_ref[i + 1, 0, own])
    total = total + (turned(tiles, 1, 0)[0] + turned(tiles, 127, 127)[0])
    return b_ref[i, 0, own] - (6.0 * tiles[0] - total) * (1.0 / factor)


class Exchange:
    def __init__(self, ref, sems, send, recv, box, depth, me, sizes):
        self.ref, self.sems, self.send, self.recv = ref, sems, send, recv
        self.c0, self.n, self.rows, self.l0, self.lanes = box
        self.depth, self.me, self.sizes = depth, me, sizes

    def _x(self):
        c0, n, depth = self.c0, self.n, self.depth
        gx = self.sizes[0]
        mx, my, mz = self.me
        rows = pl.ds(TOP, self.rows)
        out = []
        hop = 1
        slot = 0
        while (hop - 1) * n < depth and hop < gx:
            count = min(n, depth - (hop - 1) * n)
            far = (hop - 1) * n
            up = (c0 + n - count, c0 - far - count, mx + hop < gx, mx + hop, mx >= hop)
            down = (c0, c0 + n + far, mx >= hop, mx - hop, mx + hop < gx)
            for src, dst, may_send, peer, may_recv in (up, down):
                copy = pltpu.make_async_remote_copy(
                    src_ref=self.ref.at[pl.ds(src, count), 0, rows],
                    dst_ref=self.ref.at[pl.ds(dst, count), 0, rows],
                    send_sem=self.sems.at[0, slot],
                    recv_sem=self.sems.at[1, slot],
                    device_id=(peer, my, mz),
                    device_id_type=MESH,
                )
                out.append((copy, may_send, may_recv))
                slot += 1
            hop += 1
        return out

    def _y(self):
        gy = self.sizes[1]
        mx, my, mz = self.me
        planes = pl.ds(self.c0 - self.depth, self.n + 2 * self.depth)
        out = []
        up = (TOP + self.rows - PAD, TOP - PAD, my + 1 < gy, my + 1, my >= 1)
        down = (TOP, TOP + self.rows, my >= 1, my - 1, my + 1 < gy)
        for k, (src, dst, may_send, peer, may_recv) in enumerate((up, down)):
            copy = pltpu.make_async_remote_copy(
                src_ref=self.ref.at[planes, 0, pl.ds(src, PAD)],
                dst_ref=self.ref.at[planes, 0, pl.ds(dst, PAD)],
                send_sem=self.sems.at[0, 4 + k],
                recv_sem=self.sems.at[1, 4 + k],
                device_id=(mx, peer, mz),
                device_id_type=MESH,
            )
            out.append((copy, may_send, may_recv))
        return out

    def _z(self):
        gz = self.sizes[2]
        mx, my, mz = self.me
        out = []
        up = (0, mz + 1 < gz, mz + 1, mz >= 1)
        down = (1, mz >= 1, mz - 1, mz + 1 < gz)
        for k, may_send, peer, may_recv in (up, down):
            copy = pltpu.make_async_remote_copy(
                src_ref=self.send.at[k],
                dst_ref=self.recv.at[k],
                send_sem=self.sems.at[0, 6 + k],
                recv_sem=self.sems.at[1, 6 + k],
                device_id=(mx, my, peer),
                device_id_type=MESH,
            )
            out.append((copy, may_send, may_recv))
        return out

    def _start(self, copies):
        for copy, may_send, may_recv in copies:
            pl.when(may_send)(copy.start)

    def _wait(self, copies):
        for copy, may_send, may_recv in copies:
            pl.when(may_send)(copy.wait_send)
            pl.when(may_recv)(copy.wait_recv)

    def start_x(self):
        self._start(self._x())

    def wait_x(self):
        self._wait(self._x())

    def start_y(self):
        self._start(self._y())

    def wait_y(self):
        self._wait(self._y())

    def _planes(self):
        return range(self.c0 - self.depth, self.c0 + self.n + self.depth)

    def start_z(self):
        d = self.depth
        shape = self.send.shape[1:]
        lane = iota(shape, 1)
        up = jnp.zeros(shape, jnp.float32)
        down = jnp.zeros(shape, jnp.float32)
        for k, i in enumerate(self._planes()):
            v = self.ref[i, 0, PAD:PAD + shape[0]]
            here = (lane >= k * d) & (lane < k * d + d)
            up = jnp.where(here, pltpu.roll(v, (k * d - (self.l0 + self.lanes - d)) % 128, axis=1), up)
            down = jnp.where(here, pltpu.roll(v, (k * d - self.l0) % 128, axis=1), down)
        self.send[0] = up
        self.send[1] = down
        self._start(self._z())

    def wait_z(self):
        self._wait(self._z())
        d = self.depth
        gz = self.sizes[2]
        mz = self.me[2]
        shape = self.recv.shape[1:]
        lane = iota(shape, 1)
        low_at = (self.l0 - d) % 128
        high_at = (self.l0 + self.lanes) % 128
        is_low = (lane >= low_at) & (lane < low_at + d)
        is_high = (lane >= high_at) & (lane < high_at + d)
        low_buffer = jnp.where(mz >= 1, self.recv[0], 0.0)
        high_buffer = jnp.where(mz + 1 < gz, self.recv[1], 0.0)
        whole = self.ref.shape[1] == 2
        rows = slice(PAD, PAD + shape[0])
        for k, i in enumerate(self._planes()):
            low = pltpu.roll(low_buffer, (low_at - k * d) % 128, axis=1)
            high = pltpu.roll(high_buffer, (high_at - k * d) % 128, axis=1)
            if whole:
                self.ref[i, 1, rows] = jnp.where(is_low, low, jnp.where(is_high, high, 0.0))
            else:
                v = self.ref[i, 0, rows]
                self.ref[i, 0, rows] = jnp.where(is_low, low, jnp.where(is_high, high, v))


def kernel(
    sizes, rhs_ref, start_ref, out_ref,
    e0, b0, f0, e1, b1, f1, v2, b2, v3, b3,
    t0, t1, t2, t3, w0, w1, w2, pack, slots, side_send, side_recv,
    za, zb, zc, zd, ze, halo_sems, gather_sems,
):
    gx, gy, gz = sizes
    count = gx * gy * gz
    me = mx, my, mz = lax.axis_index("gx"), lax.axis_index("gy"), lax.axis_index("gz")
    mine = (mx * gy + my) * gz + mz
    lx, ly, lz = rhs_ref.shape
    c0, c1 = DOWN0 + 1, SIDE1 + 2
    hx, hy, hz = lx // 2, ly // 2, lz // 2
    qx, qy, qz = hx // 2, hy // 2, hz // 2
    x2, y2, z2 = gx * qx, gy * qy, gz * qz
    x3, y3, z3 = x2 // 2, y2 // 2, z2 // 2
    z3p = v3.shape[2]
    left = (128 - hz) // 2

    def coords(k):
        steps = (k // (gy * gz), k // gz % gy, k % gz)
        moved = [at + step for at, step in zip(me, steps)]
        return tuple(jnp.where(at >= size, at - size, at) for at, size in zip(moved, sizes))

    def number(at):
        return (at[0] * gy + at[1]) * gz + at[2]

    def others(body):
        if count <= 64:
            for k in reversed(range(1, count)):
                body(k, 0)
        else:
            lax.fori_loop(1, count, body, 0)

    for ref in (b1, f1):
        ref[...] = jnp.zeros_like(ref)
    for ref in (e0, b0, f0):
        n0 = ref.shape[0]
        ref[:, :, 0:TOP] = jnp.zeros((n0, 2, TOP, 128), jnp.float32)
        ref[:, :, TOP + ly:] = jnp.zeros((n0, 2, TOP, 128), jnp.float32)
        for i in list(range(c0)) + list(range(c0 + lx, n0)):
            ref[i] = jnp.zeros(ref.shape[1:], jnp.float32)

    barrier = pltpu.get_barrier_semaphore()

    def greet(k, carry):
        pl.semaphore_signal(barrier, inc=1, device_id=coords(k), device_id_type=MESH)
        return carry

    others(greet)

    for ref in (e1, v2, v3):
        ref[...] = jnp.zeros_like(ref)
    e0[c0:c0 + lx, 0, TOP:TOP + ly] = start_ref[...]
    b0[c0:c0 + lx, 0, TOP:TOP + ly] = rhs_ref[...]

    def code(shape, row0, lane_of, bounds):
        y = iota(shape, 0) + row0
        z = lane_of(iota(shape, 1))
        inside = (y >= 0) & (y < bounds[0]) & (z >= 0) & (z < bounds[1])
        return jnp.where(inside, (y + z) & 1, 5)

    fine = (gy * ly, gz * lz)
    t0[0] = code(t0.shape[1:], my * ly - PAD, lambda c: mz * lz + c, fine)
    t0[1] = code(t0.shape[1:], my * ly - PAD, lambda c: mz * lz + jnp.where(c < 64, c + 128, c - 128), fine)
    t1[0] = code(t1.shape[1:], my * hy - PAD, lambda c: mz * hz + c - left, (gy * hy, gz * hz))
    t2[...] = code(t2.shape, -PAD, lambda c: c, (y2, z2))
    t3[...] = code(t3.shape, -PAD, lambda c: c, (y3, z3))

    pl.semaphore_wait(barrier, count - 1)

    box0 = (c0, lx, ly, 0, lz)
    box1 = (c1, hx, hy, left, hz)
    xe0 = Exchange(e0, halo_sems.at[0], za.at[0], za.at[1], box0, DOWN0, me, sizes)
    xb0 = Exchange(b0, halo_sems.at[1], zb.at[0], zb.at[1], box0, DOWN0 - 1, me, sizes)
    xf0 = Exchange(f0, halo_sems.at[2], zc.at[0], zc.at[1], box0, SIDE0, me, sizes)
    xb1 = Exchange(b1, halo_sems.at[3], zd.at[0], zd.at[1], box1, RHS1, me, sizes)
    xf1 = Exchange(f1, halo_sems.at[4], ze.at[0], ze.at[1], box1, SIDE1, me, sizes)

    def outer(direction, k):
        return c0 + lx - k if direction == 0 else c0 + k - 1

    def halo(direction, k):
        return c0 - k if direction == 0 else c0 + lx + k - 1

    own = slice(TOP, TOP + ly)
    checks = t0[0, PAD:PAD + ly]

    def black(i):
        return checks == lax.rem(mx * lx + (i + c0 + 1), 2)

    def merged(ref, direction, k):
        i = outer(direction, k)
        return jnp.where(black(i), ref[i, 0, own], ref[outer(direction, k + 1), 0, own])

    peers = ((mx + 1 < gx, mx + 1, mx >= 1), (mx >= 1, mx - 1, mx + 1 < gx))

    def side_copies(planes, group):
        return [
            (
                pltpu.make_async_remote_copy(
                    src_ref=side_send.at[d, planes],
                    dst_ref=side_recv.at[d, planes],
                    send_sem=halo_sems.at[group, 0, d],
                    recv_sem=halo_sems.at[group, 1, d],
                    device_id=(peer, my, mz),
                    device_id_type=MESH,
                ),
                may_send,
                may_recv,
            )
            for d, (may_send, peer, may_recv) in enumerate(peers)
        ]

    near = DOWN0 - 2
    rhs_copies = [
        (
            pltpu.make_async_remote_copy(
                src_ref=rhs_ref.at[pl.ds((lx - near, 0)[d], near)],
                dst_ref=b0.at[pl.ds((c0 - near, c0 + lx)[d], near), 0, pl.ds(TOP, ly)],
                send_sem=halo_sems.at[1, 0, d],
                recv_sem=halo_sems.at[1, 1, d],
                device_id=(peer, my, mz),
                device_id_type=MESH,
            ),
            may_send,
            may_recv,
        )
        for d, (may_send, peer, may_recv) in enumerate(peers)
    ]
    for copy, may_send, may_recv in rhs_copies:
        pl.when(may_send)(copy.start)
    for d in range(2):
        side_send[d, 0] = merged(e0, d, 1)
        side_send[d, 1] = merged(e0, d, 3)
        i = outer(d, 5)
        moved = pltpu.roll(b0[outer(d, 4), 0, own], 1, axis=0)
        side_send[d, 2] = jnp.where(black(i), e0[i, 0, own], moved)
    start_copies = side_copies(pl.ds(0, 3), 0)
    xe0._start(start_copies)
    xe0._wait(start_copies)
    for d in range(2):

        @pl.when(peers[d][2])
        def _():
            for k in range(1, 5):
                e0[halo(d, k), 0, own] = side_recv[d, (k - 1) // 2]
            e0[halo(d, 5), 0, own] = side_recv[d, 2]
            b0[halo(d, 4), 0, own] = pltpu.roll(side_recv[d, 2], ly - 1, axis=0)

    xe0.start_y()
    xb0._wait(rhs_copies)
    xb0.start_y()
    xe0.wait_y()
    xe0.start_z()
    xb0.wait_y()
    xb0.start_z()
    xe0.wait_z()
    xb0.wait_z()

    def span(c, n, depth):
        return (
            jnp.maximum(c - depth, c - mx * n),
            jnp.minimum(c + n + depth, c + (gx - mx) * n),
        )

    for step in range(4):
        first, last = span(c0, lx, 4 - step)
        fine_update(e0, b0, t0, first, last, mx * lx + c0, step % 2, 1.0, CHUNK0)

    def pair0(j, carry):
        i = c0 + 2 * j
        r = fine_residual(e0, b0, i, ly, 1.0) + fine_residual(e0, b0, i + 1, ly, 1.0)
        w0[j * ly:(j + 1) * ly, :] = r
        return carry

    for j in range(hx):
        pair0(j, 0)
    r = w0[pl.ds(0, hx * hy, stride=2), :] + w0[pl.ds(1, hx * hy, stride=2), :]
    fold = jnp.where(iota((128, 128), 1) == left + iota((128, 128), 0) // 2, 0.125, 0.0)
    r = dot(r, fold)
    for j in range(hx):
        b1[c1 + j, 0, TOP:TOP + hy] = r[j * hy:(j + 1) * hy]

    xb1.start_x()
    f0[c0:c0 + lx, 0, own] = e0[c0:c0 + lx, 0, own]
    for d in range(2):
        side_send[d, 3] = merged(f0, d, 1)
        side_send[d, 4] = merged(f0, d, 3)
    side0 = side_copies(pl.ds(3, 2), 2)
    xb1.wait_x()
    xb1.start_y()
    xb1.wait_y()
    xb1.start_z()
    xb1.wait_z()

    for step in range(4):
        first, last = span(c1, hx, 4 - step)
        fine_update(e1, b1, t1, first, last, mx * hx + c1, step % 2, 4.0, CHUNK1)

    for j in range(qx):
        i = c1 + 2 * j
        w1[j, 0:hy, :] = fine_residual(e1, b1, i, hy, 4.0) + fine_residual(e1, b1, i + 1, hy, 4.0)
    r = jnp.concatenate(
        [w1[j, pl.ds(0, qy, stride=2), :] + w1[j, pl.ds(1, qy, stride=2), :] for j in range(qx)], axis=0
    )
    tiles = qx * qy // 8
    total = None
    for t in range(tiles):
        source = iota((128, 128), 0) - left
        target = iota((128, 128), 1)
        inside = (source >= 0) & (source < hz)
        fold = jnp.where(inside & (target == t * qz + source // 2), 0.125, 0.0)
        part = dot(r[8 * t:8 * t + 8], fold)
        total = part if total is None else total + part
    pack[...] = total
    slots[mine] = total

    def gather(k):
        at = coords(k)
        d = number(at)
        return pltpu.make_async_remote_copy(
            src_ref=pack,
            dst_ref=slots.at[mine],
            send_sem=gather_sems.at[0, d],
            recv_sem=gather_sems.at[1, mine],
            device_id=at,
            device_id_type=MESH,
        )

    def gather_start(k, carry):
        gather(k).start()
        return carry

    others(gather_start)

    f1[c1:c1 + hx, 0, TOP:TOP + hy] = e1[c1:c1 + hx, 0, TOP:TOP + hy]
    xf1.start_x()
    xf0._start(side0)
    b2[...] = jnp.zeros_like(b2)
    b3[...] = jnp.zeros_like(b3)

    def gather_wait(k, carry):
        at = coords(k)
        d = number(at)
        copy = pltpu.make_async_remote_copy(
            src_ref=pack,
            dst_ref=slots.at[d],
            send_sem=gather_sems.at[0, d],
            recv_sem=gather_sems.at[1, d],
            device_id=at,
            device_id_type=MESH,
        )
        copy.wait_send()
        copy.wait_recv()
        return carry

    others(gather_wait)
    xf1.wait_x()
    xf1.start_y()
    xf0._wait(side0)
    for d in range(2):

        @pl.when(peers[d][2])
        def _():
            for k in range(1, 5):
                f0[halo(d, k), 0, own] = side_recv[d, 3 + (k - 1) // 2]

    xf0.start_y()
    per = 128 // qz

    def spread(c, carry):
        cx, cy = c // gy, lax.rem(c, gy)
        lane = iota((8, 128), 1)
        for g in range(gz // per):
            parts = [slots[c * gz + g * per + q] for q in range(per)]
            for t in range(tiles):
                p, h = t // (qy // 8), t % (qy // 8)
                tile = jnp.zeros((8, 128), jnp.float32)
                for q in range(per):
                    here = (lane >= q * qz) & (lane < (q + 1) * qz)
                    tile = jnp.where(here, pltpu.roll(parts[q], ((q - t) * qz) % 128, axis=1), tile)
                rows = pl.ds(pl.multiple_of(PAD + cy * qy + 8 * h, 8), 8)
                b2[1 + cx * qx + p, rows, 128 * g:128 * (g + 1)] = tile
        return carry

    lax.fori_loop(0, gx * gy, spread, 0)

    for step in range(4):
        update(v2, b2, t2, 1, 1 + x2, 1, step % 2, 16.0, True)

    def pair2(q, carry):
        r = residual(v2, b2, 1 + 2 * q, 16.0, True) + residual(v2, b2, 2 + 2 * q, 16.0, True)
        for g in range(z2 // 128):
            w2[g] = r[:, 128 * g:128 * (g + 1)]
        half = y2 // 2
        r = jnp.concatenate(
            [
                w2[g, pl.ds(PAD, half, stride=2), :] + w2[g, pl.ds(PAD + 1, half, stride=2), :]
                for g in range(z2 // 128)
            ],
            axis=1,
        )
        fold = jnp.where(iota((z2, z3p), 1) == iota((z2, z3p), 0) // 2, 0.125, 0.0)
        b3[1 + q, PAD:PAD + half, :] = dot(r, fold)
        return carry

    for q in range(x3):
        pair2(q, 0)
    xf0.wait_y()
    xf0.start_z()
    xf1.wait_y()
    xf1.start_z()

    def sweep3(k, planes):
        for colour in (0, 1):
            now = []
            for i in range(x3):
                total = beside(planes[i], True)
                if i > 0:
                    total = total + planes[i - 1]
                if i + 1 < x3:
                    total = total + planes[i + 1]
                value = (64.0 * b3[1 + i] + total) * SIXTH
                now.append(jnp.where(t3[...] == (i + colour) % 2, value, planes[i]))
            planes = tuple(now)
        return planes

    planes = lax.fori_loop(0, CSWEEPS, sweep3, tuple(v3[1 + i] for i in range(x3)))
    for i in range(x3):
        v3[1 + i] = planes[i]

    def lift3(q, carry):
        half = (y2 + 2 * PAD) // 2
        grow = jnp.where(iota((z3p, z2), 0) == iota((z3p, z2), 1) // 2, 1.0, 0.0)
        v = dot(v3[1 + q, PAD // 2:PAD // 2 + half, :], grow)
        for g in range(z2 // 128):
            w2[g, pl.ds(0, half, stride=2), :] = v[:, 128 * g:128 * (g + 1)]
            w2[g, pl.ds(1, half, stride=2), :] = v[:, 128 * g:128 * (g + 1)]
        for g in range(z2 // 128):
            lanes = slice(128 * g, 128 * (g + 1))
            for i in (1 + 2 * q, 2 + 2 * q):
                v2[i, :, lanes] = v2[i, :, lanes] + w2[g]
        return carry

    for q in range(x3):
        lift3(q, 0)

    for step in range(4):
        update(v2, b2, t2, 1, 1 + x2, 1, step % 2, 16.0, True)

    xf1.wait_z()
    rows1 = f1.shape[2]
    grow1 = jnp.where(
        iota((z2, 128), 0) == mz * qz + (iota((z2, 128), 1) - left + 2 * 128) // 2 - 128, 1.0, 0.0
    )
    rows2 = pl.ds(pl.multiple_of(my * qy, 8), rows1 // 2)

    high2 = rows1 // 2
    window = min(x2, qx + 2 * (SIDE1 // 2))
    begin = jnp.clip(mx * qx - SIDE1 // 2, 0, x2 - window)
    v = jnp.concatenate([v2[1 + begin + k, rows2, :] for k in range(window)], axis=0)
    v = dot(v, grow1)
    for k in range(window):
        part = v[k * high2:(k + 1) * high2]
        w1[k, pl.ds(0, high2, stride=2), :] = part
        w1[k, pl.ds(1, high2, stride=2), :] = part
    for k in range(window):
        i = c1 + 2 * (begin + k) - mx * hx
        rows = slice(PAD, rows1 - PAD)
        lifted = w1[k, rows, :]
        f1[i, 0, rows] = f1[i, 0, rows] + lifted
        f1[i + 1, 0, rows] = f1[i + 1, 0, rows] + lifted

    for step in range(4):
        first, last = span(c1, hx, 5 - step)
        fine_update(f1, b1, t1, first, last, mx * hx + c1, step % 2, 4.0, CHUNK1)

    xf0.wait_z()
    grow0 = jnp.where(
        iota((128, 256), 0) == (left + iota((128, 256), 1) // 2) % 128, 1.0, 0.0
    )
    rows0 = f0.shape[2]
    half0 = rows0 // 2

    def lift1(c, carry):
        j = first + 2 * c
        v = jnp.concatenate([f1[j + k, 0, PAD:PAD + half0] for k in range(2)], axis=0)
        v = dot(v, grow0)
        for k in range(2):
            for g in range(2):
                at = pl.ds((2 * k + g) * rows0, half0, stride=2)
                w0[at, :] = v[k * half0:(k + 1) * half0, 128 * g:128 * (g + 1)]
                at = pl.ds((2 * k + g) * rows0 + 1, half0, stride=2)
                w0[at, :] = v[k * half0:(k + 1) * half0, 128 * g:128 * (g + 1)]
        for k in range(2):
            for g in range(2):
                rows = slice(PAD, rows0 - PAD)
                base = (2 * k + g) * rows0
                lifted = w0[base + PAD:base + rows0 - PAD, :]
                for i in range(2):
                    at = c0 + 2 * (j + k - c1) + i
                    f0[at, g, rows] = f0[at, g, rows] + lifted
        return carry

    first, last = span(c1, hx, SIDE0 // 2)
    lax.fori_loop(0, (last - first) // 2, lift1, 0)

    for step in range(4):
        first, last = span(c0, lx, 3 - step)
        fine_update(f0, b0, t0, first, last, mx * lx + c0, step % 2, 1.0, CHUNK0)

    out_ref[...] = f0[c0:c0 + lx, 0, own]


def local(sizes, right_side, start):
    gx, gy, gz = sizes
    lx, ly, lz = right_side.shape
    c0, c1 = DOWN0 + 1, SIDE1 + 2
    n0, n1 = lx + 2 * c0, lx // 2 + 2 * c1
    r0, r1 = ly + 2 * TOP, ly // 2 + 2 * TOP
    x2, y2, z2 = gx * lx // 4, gy * ly // 4, gz * lz // 4
    x3, y3, z3 = x2 // 2, y2 // 2, z2 // 2
    z3p = -(-z3 // 128) * 128
    f32, i32 = jnp.float32, jnp.int32
    count = gx * gy * gz
    return pl.pallas_call(
        functools.partial(kernel, sizes),
        out_shape=jax.ShapeDtypeStruct(start.shape, f32),
        in_specs=[pl.BlockSpec(memory_space=pltpu.VMEM)] * 2,
        out_specs=pl.BlockSpec(memory_space=pltpu.VMEM),
        scratch_shapes=[
            pltpu.VMEM((n0, 2, r0, 128), f32),
            pltpu.VMEM((n0, 2, r0, 128), f32),
            pltpu.VMEM((n0, 2, r0, 128), f32),
            pltpu.VMEM((n1, 1, r1, 128), f32),
            pltpu.VMEM((n1, 1, r1, 128), f32),
            pltpu.VMEM((n1, 1, r1, 128), f32),
            pltpu.VMEM((x2 + 2, y2 + 2 * PAD, z2), f32),
            pltpu.VMEM((x2 + 2, y2 + 2 * PAD, z2), f32),
            pltpu.VMEM((x3 + 2, y3 + 2 * PAD, z3p), f32),
            pltpu.VMEM((x3 + 2, y3 + 2 * PAD, z3p), f32),
            pltpu.VMEM((2, r0 - 2 * PAD, 128), i32),
            pltpu.VMEM((1, r1 - 2 * PAD, 128), i32),
            pltpu.VMEM((y2 + 2 * PAD, z2), i32),
            pltpu.VMEM((y3 + 2 * PAD, z3p), i32),
            pltpu.VMEM((max(lx // 2 * ly, 4 * r0), 128), f32),
            pltpu.VMEM((lx // 4 + SIDE1, r1, 128), f32),
            pltpu.VMEM((z2 // 128, y2 + 2 * PAD, 128), f32),
            pltpu.VMEM((8, 128), f32),
            pltpu.VMEM((count, 8, 128), f32),
            pltpu.VMEM((2, 5, ly, 128), f32),
            pltpu.VMEM((2, 5, ly, 128), f32),
            pltpu.VMEM((2, 2, r0 - 2 * PAD, 128), f32),
            pltpu.VMEM((2, 2, r0 - 2 * PAD, 128), f32),
            pltpu.VMEM((2, 2, r0 - 2 * PAD, 128), f32),
            pltpu.VMEM((2, 2, r1 - 2 * PAD, 128), f32),
            pltpu.VMEM((2, 2, r1 - 2 * PAD, 128), f32),
            pltpu.SemaphoreType.DMA((5, 2, 8)),
            pltpu.SemaphoreType.DMA((2, count)),
        ],
        compiler_params=pltpu.CompilerParams(
            collective_id=0, has_side_effects=True, vmem_limit_bytes=60 * 1024 * 1024
        ),
    )(right_side, start)


def solution(mesh):
    sizes = (mesh.shape["gx"], mesh.shape["gy"], mesh.shape["gz"])
    spec = P("gx", "gy", "gz")
    return jax.shard_map(
        functools.partial(local, sizes), mesh=mesh, in_specs=(spec, spec), out_specs=spec, check_vma=False
    )
```
